1024 devices in a mesh: gx: 128 (over z, y, core), gy: 8 (over x).
Axes of the slice: x: 8, y: 8, z: 8, core: 2. Of those that a mesh axis runs over, the one named last changes fastest.
Arguments:
- populations: float32 [27, 256, 64, 128], P(None, 'gx', 'gy'), as said below
- relax: float32 [27], replicated, may hold values from 0.6 to 1.9
- solid: int32 [256, 64, 128], P('gx', 'gy'), may hold values 0 or 1
- wall_cell: int32 [128, 8, 512], P('gx', 'gy'), may hold values from 0 to 2047, as said below
- wall_normal: int32 [128, 8, 512], P('gx', 'gy'), may hold values from 0 to 5
- wall_count: int32 [128, 8], P('gx', 'gy'), may hold values from 1 to 512, as said below
- sample_ref: int32 [128, 8, 512], P('gx', 'gy'), may hold values from 0 to 511, each once within a row
- stencil_cell: int32 [128, 8, 8, 512], P('gx', 'gy'), may hold values from 0 to 2047, as said below
- stencil_weight: float32 [128, 8, 8, 512], P('gx', 'gy'), may hold values from 0 to 1, as said below
Outputs:
- read: float32 [27, 256, 64, 128], P(None, 'gx', 'gy')
The draws below stay inside these ranges and needn't reach their ends.
Inputs may be any that keep to these rules, and one draw needn't show every extreme that they name: `populations`: positive everywhere. `wall_cell`: the 512 entries of one device are distinct local cells. Slots 0 to wall_count - 1 of a device are live; some device has all 512 live. `stencil_cell`: the eight corners of a unit cube of the owner's local cells, wrapping along z only. `stencil_weight`: nonnegative trilinear weights, summing to one over the eight corners.
All inputs are finite; a program needn't handle non-finite values. No bound on the sum of `solid` on one device may be relied on, other than what follows from the above.
Results may differ from the reference program's by a relative error of at most 0.0003.
Values sent between devices are 32-bit elements; how exact they have to be, the bound alone decides.
A program may use at most 32 MiB of HBM per device.

```python
import math
import jax
import jax.numpy as jnp
import numpy as np
from jax import lax

CX = 2
CY = 8
NZ = 128
SLOTS = 64
WALL = 512
NX = 256
NY = 64
N_GX = 128
N_GY = 8


def draw_populations(key, part):
    base = jax.random.fold_in(key, 101)
    steps = np.array([(a - 1, b - 1, c - 1) for a in range(3) for b in range(3) for c in range(3)]).T
    drift = np.array([0.06, 0.02, -0.02])
    projected = drift @ steps
    resting = 1.0 + 3.0 * projected + 4.5 * projected * projected - 1.5 * np.sum(drift * drift)
    shape = (27, NX, NY, NZ)
    noise = 0.12 * jnp.clip(jax.random.normal(base, shape, jnp.float32), -3.5, 3.5)
    return (jnp.asarray(resting, jnp.float32).reshape(27, 1, 1, 1) * (1.0 + noise)).astype(jnp.float32)


def draw_stencil_cell(key, part):
    grid_x = NX // CX
    grid_y = NY // CY
    shape = (grid_x, grid_y, 1, WALL)
    first, second, third = jax.random.split(jax.random.fold_in(key, 202), 3)
    base_x = jax.random.randint(first, shape, 0, CX - 1)
    base_y = jax.random.randint(second, shape, 0, CY - 1)
    base_z = jax.random.randint(third, shape, 0, NZ)
    corner = jnp.arange(8, dtype=jnp.int32).reshape(1, 1, 8, 1)
    offset_x = corner // 4
    offset_y = corner // 2 % 2
    offset_z = corner % 2
    cells = ((base_x + offset_x) * CY + base_y + offset_y) * NZ + (base_z + offset_z) % NZ
    return cells.astype(jnp.int32)


def draw_stencil_weight(key, part):
    grid_x = NX // CX
    grid_y = NY // CY
    shape = (grid_x, grid_y, 3, 1, WALL)
    base = jax.random.fold_in(key, 303)
    fraction = jax.random.uniform(base, shape, jnp.float32, 0.0, 1.0)
    corner = jnp.arange(8, dtype=jnp.int32)
    bits = jnp.stack([corner // 4, corner // 2 % 2, corner % 2]).reshape(1, 1, 3, 8, 1)
    factor = jnp.where(bits == 1, fraction, 1.0 - fraction)
    return jnp.prod(factor, axis=2).astype(jnp.float32)


def draw_wall_cell(key, part):
    grid_x = NX // CX
    grid_y = NY // CY
    keys = jax.random.split(jax.random.fold_in(key, 404), grid_x * grid_y)
    chosen = jax.vmap(lambda item: jax.random.permutation(item, CX * CY * NZ)[:WALL])(keys)
    return chosen.reshape(grid_x, grid_y, WALL).astype(jnp.int32)


def draw_wall_count(key, part):
    grid_x = NX // CX
    grid_y = NY // CY
    shifted = jax.random.randint(jax.random.fold_in(key, 505), (grid_x, grid_y), 0, 4)
    counts = jnp.right_shift(jnp.full((grid_x, grid_y), WALL, jnp.int32), shifted.astype(jnp.int32))
    counts = jnp.maximum(counts, 1).at[0, 0].set(WALL)
    return counts.astype(jnp.int32)


def plant(result, rng, smallest, top_value):
    dims = result.shape
    spot = [jax.random.randint(jax.random.fold_in(rng, axis), (), 0, dims[axis]) for axis in range(len(dims))]
    result = result.at[tuple(spot)].set(smallest)
    longest = dims.index(max(dims))
    spot[longest] = (spot[longest] + 1) % dims[longest]
    return result.at[tuple(spot)].set(top_value)


def setup_inputs(seed: int = 0) -> dict:
    arg_keys = jax.random.split(jax.random.key(seed), 10)
    populations = draw_populations(jax.random.fold_in(arg_keys[9], 71), 0)
    relax = jnp.clip(jnp.exp(jax.random.uniform(arg_keys[1], (27,), jnp.float32, math.log(0.6), math.log(1.9))), 0.6, 1.9)
    solid = plant((jax.random.randint(arg_keys[2], (NX, NY, NZ), 0, 8) < 1).astype(jnp.int32), jax.random.fold_in(arg_keys[2], 1), 0, 1)
    wall_cell = draw_wall_cell(jax.random.fold_in(arg_keys[9], 71), 0)
    wall_normal = plant(jax.random.randint(arg_keys[4], (N_GX, N_GY, WALL), 0, 6), jax.random.fold_in(arg_keys[4], 1), 0, 5).astype(jnp.int32)
    wall_count = draw_wall_count(jax.random.fold_in(arg_keys[9], 71), 0)
    sample_ref = jax.vmap(lambda own: jax.random.permutation(own, WALL))(jax.random.split(arg_keys[6], N_GX * N_GY)).reshape((N_GX, N_GY, WALL)).astype(jnp.int32)
    stencil_cell = draw_stencil_cell(jax.random.fold_in(arg_keys[9], 71), 0)
    stencil_weight = draw_stencil_weight(jax.random.fold_in(arg_keys[9], 71), 0)
    return {"populations": populations, "relax": relax, "solid": solid, "wall_cell": wall_cell, "wall_normal": wall_normal, "wall_count": wall_count, "sample_ref": sample_ref, "stencil_cell": stencil_cell, "stencil_weight": stencil_weight}


lattice_steps = [(a - 1, b - 1, c - 1) for a in range(3) for b in range(3) for c in range(3)]
wall_ratio = (1.0 / 9.0) ** (1.0 / 7.0)


def lattice():
    steps = np.array(lattice_steps).T
    single = np.where(steps == 0, 2.0 / 3.0, 1.0 / 6.0)
    weights = np.prod(single, axis=0)
    vander = np.array([[1.0, 1.0, 1.0], [-1.0, 0.0, 1.0], [1.0, 0.0, 1.0]])
    undo = np.array([[0.0, -0.5, 0.5], [1.0, 0.0, -1.0], [0.0, 0.5, 0.5]])
    moment = np.kron(np.kron(vander, vander), vander)
    inverse = np.kron(np.kron(undo, undo), undo)
    return (jnp.asarray(steps, jnp.float32), jnp.asarray(weights, jnp.float32),
            jnp.asarray(moment, jnp.float32), jnp.asarray(inverse, jnp.float32))


def moments(pops):
    steps, weights, moment, inverse = lattice()
    scaled = weights[:, None] * pops
    density = jnp.sum(scaled, axis=0)
    momentum = jnp.dot(steps, scaled, precision=lax.Precision.HIGHEST)
    return density, momentum / density[None]


def equilibrium(density, velocity):
    steps, weights, moment, inverse = lattice()
    projected = jnp.dot(steps.T, velocity, precision=lax.Precision.HIGHEST)
    speed_sq = jnp.sum(velocity * velocity, axis=0)
    return density[None] * (1.0 + 3.0 * projected + 4.5 * projected * projected - 1.5 * speed_sq[None])


def collide(pops, relax):
    steps, weights, moment, inverse = lattice()
    scaled = weights[:, None] * pops
    density, velocity = moments(pops)
    balance = weights[:, None] * equilibrium(density, velocity)
    deviation = jnp.dot(moment, scaled - balance, precision=lax.Precision.HIGHEST) * relax[:, None]
    after = scaled - jnp.dot(inverse, deviation, precision=lax.Precision.HIGHEST)
    return after / weights[:, None]


def sample_velocity(velocity, corner_cells, corner_weight):
    picked = velocity[:, corner_cells]
    return jnp.sum(picked * corner_weight[None], axis=1)


def rebuild_columns(columns, density, velocity, normal, live, picked):
    axis_index = normal // 2
    sign = (2 * (normal % 2) - 1).astype(jnp.float32)
    normal_vec = (jnp.arange(3, dtype=jnp.int32)[:, None] == axis_index[None]).astype(jnp.float32) * sign[None]
    along = jnp.sum(picked * normal_vec, axis=0)
    tangential = picked - along[None] * normal_vec
    wall_eq = equilibrium(density, wall_ratio * tangential)
    local_eq = equilibrium(density, velocity)
    return jnp.where(live[None], wall_eq + columns - local_eq, columns)


def rebuild_block(block, density, velocity, cells, normal, live, picked):
    columns = rebuild_columns(block[:, cells], density[cells], velocity[:, cells], normal, live, picked)
    return block.at[:, cells].set(columns)


def to_blocks(field):
    count = field.shape[0]
    field = field.reshape(count, N_GX, CX, N_GY, CY, NZ).transpose(1, 3, 0, 2, 4, 5)
    return field.reshape(N_GX, N_GY, count, CX * CY * NZ)


def from_blocks(blocks):
    count = blocks.shape[2]
    field = blocks.reshape(N_GX, N_GY, count, CX, CY, NZ).transpose(2, 0, 3, 1, 4, 5)
    return field.reshape(count, N_GX * CX, N_GY * CY, NZ)


def reference(populations, relax, solid, wall_cell, wall_normal, wall_count, sample_ref, stencil_cell, stencil_weight):
    blocks = to_blocks(populations)
    density_b, velocity_b = lax.map(lambda row: jax.vmap(moments)(row), blocks)
    samples = jax.vmap(jax.vmap(sample_velocity))(velocity_b, stencil_cell, stencil_weight)
    sent = samples.reshape(N_GX, N_GY, 3, N_GY, SLOTS)
    received = sent.transpose(0, 3, 2, 1, 4).reshape(N_GX, N_GY, 3, N_GY * SLOTS)
    picked = jax.vmap(jax.vmap(lambda table, where_from: table[:, where_from]))(received, sample_ref)
    live = jnp.arange(N_GY * SLOTS, dtype=jnp.int32)[None, None, :] < wall_count[:, :, None]
    rebuilt = jax.vmap(jax.vmap(rebuild_block))(blocks, density_b, velocity_b, wall_cell, wall_normal, live, picked)
    post_b = lax.map(lambda row: jax.vmap(lambda block: collide(block, relax))(row), rebuilt)
    post = from_blocks(post_b)
    outputs = []
    for direction in range(27):
        step_x, step_y, step_z = lattice_steps[direction]
        moved = jnp.roll(post[direction], (step_x, step_y, step_z), axis=(0, 1, 2))
        blocked = jnp.roll(solid, (step_x, step_y, step_z), axis=(0, 1, 2))
        outputs.append(jnp.where(blocked != 0, post[26 - direction], moved))
    return jnp.stack(outputs)
```

```python
import jax
import jax.numpy as jnp
import numpy as np
from jax import lax
from jax.experimental import pallas as pl
from jax.experimental.pallas import tpu as pltpu
from jax.sharding import PartitionSpec as P

MESH = pl.DeviceIdType.MESH
wall_ratio = (1.0 / 9.0) ** (1.0 / 7.0)
steps = [(a, b, c) for a in (-1, 0, 1) for b in (-1, 0, 1) for c in (-1, 0, 1)]
index_of = {e: i for i, e in enumerate(steps)}
weight = [float(np.prod([2.0 / 3.0 if v == 0 else 1.0 / 6.0 for v in e])) for e in steps]
F32 = jnp.float32
I32 = jnp.int32


def along(values, axis, combine):
    stride = (9, 3, 1)[axis]
    out = list(values)
    for i in range(27):
        if i // stride % 3 == 0:
            out[i], out[i + stride], out[i + 2 * stride] = combine(
                values[i], values[i + stride], values[i + 2 * stride]
            )
    return out


def to_moments(lo, mid, hi):
    both = hi + lo
    return both + mid, hi - lo, both


def from_moments(zero, one, two):
    return two - one, zero - two, two + one


def equilibrium_moments(rho, vel):
    sq = [v * v for v in vel]
    third = 1.0 / 3.0
    out = []
    for powers in [(a, b, c) for a in range(3) for b in range(3) for c in range(3)]:
        odd = [k for k in range(3) if powers[k] == 1]
        even = [k for k in range(3) if powers[k] == 2]
        scale = third ** len(even)
        if len(odd) == 3:
            out.append(None)
        elif len(odd) == 2:
            out.append(rho * (vel[odd[0]] * vel[odd[1]] * scale))
        elif len(odd) == 1:
            out.append(rho * (vel[odd[0]] * scale))
        elif not even:
            out.append(rho)
        else:
            total = sq[even[0]]
            for k in even[1:]:
                total = total + sq[k]
            out.append(rho * (scale + 3.0 * scale * total))
    return out


def shifted(value, b, c):
    if c:
        value = pltpu.roll(value, c % 128, 1)
    if b:
        value = pltpu.roll(value, b % 8, 0)
    return value


def lane_gather(table, index):
    return jnp.take_along_axis(table, index, axis=1, mode="promise_in_bounds")


def row_of(ref, lead, row):
    return jnp.broadcast_to(ref[lead + (slice(row, row + 1), slice(None))], (8, 128))


def body(
    n_gx,
    n_gy,
    pop_h,
    relax_s,
    solid_h,
    cell_h,
    normal_h,
    count_s,
    ref_h,
    corner_h,
    cweight_h,
    out,
    pop,
    solid,
    cell,
    normal,
    sref,
    corner,
    cweight,
    part,
    fields,
    code,
    blocked,
    sample,
    sample_in,
    solid_x,
    solid_y,
    solid_d,
    face,
    face_in,
    rows,
    rows_in,
    rows_d,
    rolled,
    posts,
    in_sem,
    s_send,
    s_recv,
    o_send,
    o_recv,
    h_send,
    h_recv,
):
    p = lax.axis_index("gx")
    q = lax.axis_index("gy")
    px = [lax.rem(p + n_gx + a, n_gx) for a in (-1, 0, 1)]
    qy = [lax.rem(q + n_gy + b, n_gy) for b in (-1, 0, 1)]

    loads = [
        pltpu.make_async_copy(src, dst, in_sem.at[k])
        for k, (src, dst) in enumerate(
            [
                (pop_h, pop),
                (corner_h, corner),
                (cweight_h, cweight),
                (solid_h, solid),
                (cell_h, cell),
                (normal_h, normal),
                (ref_h, sref),
            ]
        )
    ]
    for copy in loads:
        copy.start()

    barrier = pltpu.get_barrier_semaphore()
    ring = [(p, lax.rem(q + k, n_gy)) for k in range(1, n_gy)]
    side = [(px[a + 1], qy[b + 1]) for a in (-1, 1) for b in (-1, 0, 1)]
    for peer in ring + side:
        pl.semaphore_signal(barrier, inc=1, device_id=peer, device_id_type=MESH)

    row_id = lax.broadcasted_iota(I32, (8, 128), 0)

    loads[0].wait()
    vel = []
    for x in range(2):
        f = [pop[i, x] * weight[i] for i in range(27)]
        for axis in (2, 1, 0):
            f = along(f, axis, to_moments)
        rho = f[0]
        inv = 1.0 / rho
        u = [f[9] * inv, f[3] * inv, f[1] * inv]
        vel.append(u)
        fields[0, x] = rho
        for k in range(3):
            fields[k + 1, x] = u[k]
        balance = equilibrium_moments(rho, u)
        for m in range(27):
            off = f[m] if balance[m] is None else f[m] - balance[m]
            f[m] = off * (1.0 - relax_s[m])
        for axis in (2, 1, 0):
            f = along(f, axis, from_moments)
        for i, e in enumerate(steps):
            part[i, x] = f[i] * float(np.prod([1.5 if v == 0 else 3.0 for v in e]))

    loads[1].wait()
    loads[2].wait()
    for j in range(4):
        total = [jnp.zeros((8, 128), F32) for _ in range(3)]
        lanes = slice(128 * j, 128 * (j + 1))
        for k in range(8):
            where = jnp.broadcast_to(corner[0, 0, k : k + 1, lanes], (8, 128))
            share = jnp.broadcast_to(cweight[0, 0, k : k + 1, lanes], (8, 128))
            lane = where & 127
            mine = jnp.where((where >> 7) & 7 == row_id, share, 0.0)
            upper = where >= 1024
            for n in range(3):
                got = jnp.where(upper, lane_gather(vel[1][n], lane), lane_gather(vel[0][n], lane))
                total[n] = total[n] + mine * got
        for n in range(3):
            sample[j, n : n + 1] = jnp.sum(total[n], axis=0, keepdims=True)

    pl.semaphore_wait(barrier, len(ring) + len(side))

    def send(src, dst, send_sem, recv_sem, peer):
        copy = pltpu.make_async_remote_copy(
            src_ref=src, dst_ref=dst, send_sem=send_sem, recv_sem=recv_sem,
            device_id=peer, device_id_type=MESH,
        )
        copy.start()
        return copy

    sample_copies = [
        send(sample.at[peer[1] // 2], sample_in.at[q], s_send.at[k], s_recv.at[q], peer)
        for k, peer in enumerate(ring)
    ]
    loads[3].wait()
    solid_copies = []
    for n, a in enumerate((1, -1)):
        mine = 1 if a == 1 else 0
        solid_copies.append(
            send(solid.at[mine], solid_x.at[n], o_send.at[n], o_recv.at[n], (px[a + 1], q))
        )
        solid_copies.append(
            send(solid, solid_y.at[n], o_send.at[2 + n], o_recv.at[2 + n], (p, qy[a + 1]))
        )
        for m, b in enumerate((1, -1)):
            k = 4 + 2 * n + m
            solid_copies.append(
                send(solid.at[mine], solid_d.at[n, m], o_send.at[k], o_recv.at[k], (px[a + 1], qy[b + 1]))
            )

    for k in range(4, 7):
        loads[k].wait()
    cells = cell[0]
    live = lax.broadcasted_iota(I32, (1, 512), 1) < count_s[0, 0]
    refs = sref[0]
    first = jnp.where(live, (refs & 63) + 1, 0)
    second = jnp.where(live, (refs >> 6) * 8 + normal[0], 0)
    rows16 = lax.broadcasted_iota(I32, (16, 512), 0) == (cells >> 7)
    left = jnp.concatenate(
        [jnp.where(rows16, first, 0), jnp.where(rows16, second, 0)], axis=0
    ).astype(F32).astype(jnp.bfloat16)
    right = jnp.where(
        lax.broadcasted_iota(I32, (128, 512), 0) == (cells & 127), 1.0, 0.0
    ).astype(jnp.bfloat16)
    code[...] = lax.dot_general(
        left, right, (((1,), (1,)), ((), ())), preferred_element_type=F32
    ).astype(I32)

    for copy in solid_copies:
        copy.wait_recv()
    flags = [solid_x[0], solid[0], solid[1], solid_x[1]]
    for xx in range(4):
        for b in (-1, 0, 1):
            plane = flags[xx]
            if b:
                m = 0 if b == 1 else 1
                near = 7 if b == 1 else 0
                if xx in (1, 2):
                    edge = row_of(solid_y, (m, xx - 1), near)
                else:
                    edge = row_of(solid_d, (0 if xx == 0 else 1, m), near)
                plane = pltpu.roll(plane, b % 8, 0)
                plane = jnp.where(row_id == (0 if b == 1 else 7), edge, plane)
            for c in (-1, 0, 1):
                blocked[xx, 3 * (b + 1) + c + 1] = shifted(plane, 0, c)

    for copy in sample_copies:
        copy.wait_send()
    for k in range(1, n_gy):
        peer = lax.rem(q + n_gy - k, n_gy)
        pltpu.make_async_remote_copy(
            src_ref=sample.at[0], dst_ref=sample_in.at[peer], send_sem=s_send.at[0],
            recv_sem=s_recv.at[peer], device_id=(p, peer), device_id_type=MESH,
        ).wait_recv()
    sample_in[q] = sample[q // 2]

    lane_base = lax.rem(q, 2) * 64 - 1
    for x in range(2):
        first = code[8 * x : 8 * x + 8]
        second = code[16 + 8 * x : 24 + 8 * x]
        lane = jnp.maximum(first + lane_base, 0)
        owner = second >> 3
        axis = (second & 7) >> 1
        picked = [jnp.zeros((8, 128), F32) for _ in range(3)]
        for k in range(n_gy):
            here = owner == k
            for n in range(3):
                got = lane_gather(row_of(sample_in, (k,), n), lane)
                picked[n] = jnp.where(here, got, picked[n])
        rho = fields[0, x]
        u = [
            jnp.where(
                first > 0,
                jnp.where(axis == n, 0.0, wall_ratio * picked[n]),
                fields[n + 1, x],
            )
            for n in range(3)
        ]
        base = rho - 1.5 * rho * (u[0] * u[0] + u[1] * u[1] + u[2] * u[2])
        for i in range(13, 27):
            e = steps[i]
            along_e = None
            for n in range(3):
                if e[n]:
                    term = u[n] if e[n] > 0 else -u[n]
                    along_e = term if along_e is None else along_e + term
            if along_e is None:
                posts[i, x] = part[i, x] + base
                continue
            linear = 3.0 * rho * along_e
            even = base + 1.5 * along_e * linear
            posts[i, x] = part[i, x] + (even + linear)
            posts[26 - i, x] = part[26 - i, x] + (even - linear)

    for i, (a, b, c) in enumerate(steps):
        for x in range(2):
            value = shifted(posts[i, x], b, c)
            inside = 0 <= x + a <= 1
            if inside:
                rolled[i, x] = value
            else:
                face[0 if a == 1 else 1, 3 * (b + 1) + c + 1] = value
            if b:
                m = 0 if b == 1 else 1
                near = 0 if b == 1 else 7
                if inside:
                    r = 4 * (c + 1) + (x if a == 0 else 2 if a == 1 else 3)
                else:
                    r = (16 if a == 1 else 24) + c + 1
                rows[m, r : r + 1] = value[near : near + 1]

    halo_copies = []
    for n, a in enumerate((1, -1)):
        for m, b in enumerate((1, -1)):
            k = 4 + 2 * n + m
            halo_copies.append(
                send(rows.at[m, pl.ds(16 + 8 * n, 8)], rows_d.at[n, m], h_send.at[k], h_recv.at[k],
                     (px[a + 1], qy[b + 1]))
            )
        halo_copies.append(
            send(face.at[n], face_in.at[n], h_send.at[n], h_recv.at[n], (px[a + 1], q))
        )
        halo_copies.append(
            send(rows.at[n, pl.ds(0, 16)], rows_in.at[n], h_send.at[2 + n], h_recv.at[2 + n],
                 (p, qy[a + 1]))
        )
    for copy in halo_copies:
        copy.wait_recv()

    for i, (a, b, c) in enumerate(steps):
        for x in range(2):
            from_x = x - a
            inside = 0 <= from_x <= 1
            n = 0 if a == 1 else 1
            value = rolled[i, from_x] if inside else face_in[n, 3 * (b + 1) + c + 1]
            if b:
                m = 0 if b == 1 else 1
                if inside:
                    r = 4 * (c + 1) + (from_x if a == 0 else 2 if a == 1 else 3)
                    edge = row_of(rows_in, (m,), r)
                else:
                    edge = row_of(rows_d, (n, m), c + 1)
                value = jnp.where(row_id == (0 if b == 1 else 7), edge, value)
            wall = blocked[from_x + 1, 3 * (b + 1) + c + 1]
            out[i, x] = jnp.where(wall != 0, posts[26 - i, x], value)

    for copy in solid_copies + halo_copies:
        copy.wait_send()


def local(*args):
    n_gx, n_gy = lax.axis_size("gx"), lax.axis_size("gy")
    hbm = pl.BlockSpec(memory_space=pl.ANY)
    smem = pl.BlockSpec(memory_space=pltpu.SMEM)
    vmem = pltpu.VMEM
    dma = pltpu.SemaphoreType.DMA
    return pl.pallas_call(
        lambda *refs: body(n_gx, n_gy, *refs),
        name="lattice_step",
        out_shape=jax.ShapeDtypeStruct((27, 2, 8, 128), F32),
        in_specs=[hbm, smem, hbm, hbm, hbm, smem, hbm, hbm, hbm],
        out_specs=pl.BlockSpec(memory_space=pltpu.VMEM),
        scratch_shapes=[
            vmem((27, 2, 8, 128), F32),
            vmem((2, 8, 128), I32),
            vmem((1, 1, 512), I32),
            vmem((1, 1, 512), I32),
            vmem((1, 1, 512), I32),
            vmem((1, 1, 8, 512), I32),
            vmem((1, 1, 8, 512), F32),
            vmem((27, 2, 8, 128), F32),
            vmem((4, 2, 8, 128), F32),
            vmem((32, 128), I32),
            vmem((4, 9, 8, 128), I32),
            vmem((4, 8, 128), F32),
            vmem((n_gy, 8, 128), F32),
            vmem((2, 8, 128), I32),
            vmem((2, 2, 8, 128), I32),
            vmem((2, 2, 8, 128), I32),
            vmem((2, 9, 8, 128), F32),
            vmem((2, 9, 8, 128), F32),
            vmem((2, 32, 128), F32),
            vmem((2, 16, 128), F32),
            vmem((2, 2, 8, 128), F32),
            vmem((27, 2, 8, 128), F32),
            vmem((27, 2, 8, 128), F32),
            dma((7,)),
            dma((n_gy - 1,)),
            dma((n_gy,)),
            dma((8,)),
            dma((8,)),
            dma((8,)),
            dma((8,)),
        ],
        compiler_params=pltpu.CompilerParams(collective_id=0, has_side_effects=True),
    )(*args)


def solution(mesh):
    return jax.shard_map(
        local,
        mesh=mesh,
        in_specs=(
            P(None, "gx", "gy", None),
            P(),
            P("gx", "gy", None),
            P("gx", "gy", None),
            P("gx", "gy", None),
            P("gx", "gy"),
            P("gx", "gy", None),
            P("gx", "gy", None, None),
            P("gx", "gy", None, None),
        ),
        out_specs=P(None, "gx", "gy", None),
        check_vma=False,
    )
```

```python
import jax
import jax.numpy as jnp
import numpy as np
from jax import lax
from jax.experimental import pallas as pl
from jax.experimental.pallas import tpu as pltpu
from jax.sharding import PartitionSpec as P

MESH = pl.DeviceIdType.MESH
wall_ratio = (1.0 / 9.0) ** (1.0 / 7.0)
steps = [(a, b, c) for a in (-1, 0, 1) for b in (-1, 0, 1) for c in (-1, 0, 1)]
index_of = {e: i for i, e in enumerate(steps)}
weight = [float(np.prod([2.0 / 3.0 if v == 0 else 1.0 / 6.0 for v in e])) for e in steps]
F32 = jnp.float32
I32 = jnp.int32


def along(values, axis, combine):
    stride = (9, 3, 1)[axis]
    out = list(values)
    for i in range(27):
        if i // stride % 3 == 0:
            out[i], out[i + stride], out[i + 2 * stride] = combine(
                values[i], values[i + stride], values[i + 2 * stride]
            )
    return out


def to_moments(lo, mid, hi):
    both = hi + lo
    return both + mid, hi - lo, both


def from_moments(zero, one, two):
    return two - one, zero - two, two + one


def equilibrium_moments(rho, vel):
    sq = [v * v for v in vel]
    third = 1.0 / 3.0
    out = []
    for powers in [(a, b, c) for a in range(3) for b in range(3) for c in range(3)]:
        odd = [k for k in range(3) if powers[k] == 1]
        even = [k for k in range(3) if powers[k] == 2]
        scale = third ** len(even)
        if len(odd) == 3:
            out.append(None)
        elif len(odd) == 2:
            out.append(rho * (vel[odd[0]] * vel[odd[1]] * scale))
        elif len(odd) == 1:
            out.append(rho * (vel[odd[0]] * scale))
        elif not even:
            out.append(rho)
        else:
            total = sq[even[0]]
            for k in even[1:]:
                total = total + sq[k]
            out.append(rho * (scale + 3.0 * scale * total))
    return out


def shifted(value, b, c):
    if c:
        value = pltpu.roll(value, c % 128, 1)
    if b:
        value = pltpu.roll(value, b % 8, 0)
    return value


def lane_gather(table, index):
    return jnp.take_along_axis(table, index, axis=1, mode="promise_in_bounds")


def row_of(ref, lead, row):
    return jnp.broadcast_to(ref[lead + (slice(row, row + 1), slice(None))], (8, 128))


def line(ref, row):
    return jnp.broadcast_to(ref[row], (8, 128))


def total_of(u, e):
    total = None
    for n in range(3):
        if e[n]:
            term = u[n] if e[n] > 0 else -u[n]
            total = term if total is None else total + term
    return total


def body(
    n_gx,
    n_gy,
    pop_h,
    relax_h,
    solid_h,
    cell_h,
    normal_h,
    count_s,
    ref_h,
    corner_h,
    cweight_h,
    out,
    relax_s,
    pop,
    solid,
    cell,
    normal,
    sref,
    corner,
    cweight,
    part,
    fields,
    blocked,
    sample,
    sample_in,
    solid_x,
    solid_y,
    solid_d,
    part_in,
    fields_in,
    rows,
    rows_in,
    rows_d,
    rolled,
    posts,
    edges,
    in_sem,
    s_send,
    s_recv,
    h_send,
    h_recv,
):
    p = lax.axis_index("gx")
    q = lax.axis_index("gy")
    px = [lax.rem(p + n_gx + a, n_gx) for a in (-1, 0, 1)]
    qy = [lax.rem(q + n_gy + b, n_gy) for b in (-1, 0, 1)]
    around = [lax.rem(q + k, n_gy) for k in range(n_gy)]

    barrier = pltpu.get_barrier_semaphore()
    by_distance = sorted(range(n_gy), key=lambda k: -min(k, n_gy - k))
    targets = [(a, k) for a in (1, 0, -1) for k in by_distance if a or k]
    for a, k in targets:
        pl.semaphore_signal(
            barrier, inc=1, device_id=(px[a + 1], around[k]), device_id_type=MESH
        )

    loads = [
        pltpu.make_async_copy(src, dst, in_sem.at[k])
        for k, (src, dst) in enumerate(
            [
                (pop_h, pop),
                (relax_h, relax_s),
                (corner_h, corner),
                (cweight_h, cweight),
                (cell_h, cell),
                (normal_h, normal),
                (ref_h, sref),
                (solid_h, solid),
            ]
        )
    ]
    for copy in loads:
        copy.start()
    row_id = lax.broadcasted_iota(I32, (8, 128), 0)

    for copy in loads[:7]:
        copy.wait()

    cells = cell[0]
    live = lax.broadcasted_iota(I32, (1, 512), 1) < count_s[0, 0]
    refs = sref[0]
    first = jnp.where(live, (refs & 63) + 1, 0)
    second = jnp.where(live, (refs >> 6) * 8 + normal[0], 0)
    rows16 = lax.broadcasted_iota(I32, (16, 512), 0) == (cells >> 7)
    left = jnp.concatenate(
        [jnp.where(rows16, first, 0), jnp.where(rows16, second, 0)], axis=0
    ).astype(F32).astype(jnp.bfloat16)
    right = jnp.where(
        lax.broadcasted_iota(I32, (128, 512), 0) == (cells & 127), 1.0, 0.0
    ).astype(jnp.bfloat16)
    code = lax.dot_general(
        left, right, (((1,), (1,)), ((), ())), preferred_element_type=F32
    ).astype(I32)
    slot = code[0:16]
    owner = code[16:32]
    use = jnp.where(slot > 0, (owner >> 3) * 64 + slot, 0).astype(F32)
    axes = ((owner & 7) >> 1).astype(F32)
    for x in range(2):
        fields[4, x] = use[8 * x : 8 * x + 8]
        fields[5, x] = axes[8 * x : 8 * x + 8]

    vel = []
    for x in range(2):
        f = [pop[i, x] * weight[i] for i in range(27)]
        for axis in (2, 1, 0):
            f = along(f, axis, to_moments)
        rho = f[0]
        inv = 1.0 / rho
        u = [f[9] * inv, f[3] * inv, f[1] * inv]
        vel.append(u)
        fields[0, x] = rho
        for k in range(3):
            fields[k + 1, x] = u[k]
        balance = equilibrium_moments(rho, u)
        for m in range(27):
            off = f[m] if balance[m] is None else f[m] - balance[m]
            f[m] = off * (1.0 - relax_s[m])
        for axis in (2, 1, 0):
            f = along(f, axis, from_moments)
        for i, e in enumerate(steps):
            part[i, x] = f[i] * float(np.prod([1.5 if v == 0 else 3.0 for v in e]))

    for j in range(4):
        total = [jnp.zeros((8, 128), F32) for _ in range(3)]
        lanes = slice(128 * j, 128 * (j + 1))
        for k in range(8):
            where = jnp.broadcast_to(corner[0, 0, k : k + 1, lanes], (8, 128))
            share = jnp.broadcast_to(cweight[0, 0, k : k + 1, lanes], (8, 128))
            lane = where & 127
            mine = jnp.where((where >> 7) & 7 == row_id, share, 0.0)
            upper = where >= 1024
            for n in range(3):
                got = jnp.where(upper, lane_gather(vel[1][n], lane), lane_gather(vel[0][n], lane))
                total[n] = total[n] + mine * got
        for n in range(3):
            summed = jnp.sum(total[n], axis=0, keepdims=True)
            sample[3 * j + n] = summed
            if j == 0:
                sample[12 + n] = summed

    for m, b in enumerate((1, -1)):
        near = slice(7, 8) if b == 1 else slice(0, 1)
        base = 42 * m
        for c in (-1, 0, 1):
            for s, (a, x) in enumerate(((0, 0), (0, 1), (1, 0), (-1, 1))):
                rows[base + 4 * (c + 1) + s] = part[index_of[a, b, c], x, near]
            for n, (a, x) in enumerate(((1, 1), (-1, 0))):
                rows[base + 24 + 9 * n + c + 1] = part[index_of[a, b, c], x, near]
        for k in range(6):
            for x in range(2):
                value = fields[k, x, near]
                rows[base + 12 + 6 * x + k] = value
                rows[base + 27 + 9 * (1 - x) + k] = value

    par = lax.rem(q, 2)

    def window(d):
        return 3 * lax.div(lax.rem(d + n_gy - 1, n_gy), 2)

    mine = window(q)
    for r in range(6):
        sample_in[(n_gy + q) * 6 + r] = sample[mine + r]

    loads[7].wait()
    pl.semaphore_wait(barrier, len(targets))

    def send(src, dst, send_sem, recv_sem, peer):
        copy = pltpu.make_async_remote_copy(
            src_ref=src, dst_ref=dst, send_sem=send_sem, recv_sem=recv_sem,
            device_id=peer, device_id_type=MESH,
        )
        copy.start()
        return copy

    def send_samples(a):
        return [
            send(
                sample.at[pl.ds(window(around[k]), 6)],
                sample_in.at[pl.ds(((1 - a) * n_gy + q) * 6, 6)],
                s_send.at[t],
                s_recv.at[(1 - a) * n_gy + q],
                (px[a + 1], around[k]),
            )
            for t, (b, k) in enumerate(targets)
            if b == a
        ]

    def send_side(n):
        a = 1 - 2 * n
        x = 1 - n
        to = px[a + 1]
        halo = []
        for m, b in enumerate((1, -1)):
            halo.append(
                (rows.at[pl.ds(42 * m + 24 + 9 * n, 9)], rows_d.at[pl.ds((2 * n + m) * 9, 9)], (to, qy[b + 1]))
            )
        halo.append((fields.at[:, x], fields_in.at[n], (to, q)))
        halo.append((part.at[pl.ds(18 - 18 * n, 9), x], part_in.at[n], (to, q)))
        halo.append((solid.at[x], solid_x.at[n], (to, q)))
        for m, b in enumerate((1, -1)):
            halo.append((solid.at[x], solid_d.at[n, m], (to, qy[b + 1])))
        return [
            send(src, dst, h_send.at[7 * n + k], h_recv.at[7 * n + k], peer)
            for k, (src, dst, peer) in enumerate(halo)
        ]

    def send_row():
        halo = []
        for m, b in enumerate((1, -1)):
            to = (p, qy[b + 1])
            halo.append((rows.at[pl.ds(42 * m, 24)], rows_in.at[pl.ds(24 * m, 24)], to))
            halo.append((solid, solid_y.at[m], to))
        return [
            send(src, dst, h_send.at[14 + k], h_recv.at[14 + k], peer)
            for k, (src, dst, peer) in enumerate(halo)
        ]

    sent = send_samples(1)
    up = send_side(0)
    sent = sent + send_samples(0)
    row = send_row()
    sent = sent + send_samples(-1)
    down = send_side(1)

    def received(g, k):
        pltpu.make_async_remote_copy(
            src_ref=sample.at[pl.ds(0, 6)],
            dst_ref=sample_in.at[pl.ds((g * n_gy + around[k]) * 6, 6)],
            send_sem=s_send.at[0],
            recv_sem=s_recv.at[g * n_gy + around[k]],
            device_id=(p, around[k]),
            device_id_type=MESH,
        ).wait_recv()

    chunk = [0, 1 - par, 1]
    half = [1 - par, par, 1 - par]

    def table(g, t, k, n):
        return line(sample_in, (g * n_gy + around[k]) * 6 + 3 * chunk[t] + n)

    def wall_velocity(use, axis, u, tables, lanes):
        use = use.astype(I32)
        spot = use - 1
        who = spot >> 6
        lane = (spot & 63) + lanes
        picked = [jnp.zeros((8, 128), F32) for _ in range(3)]
        for k in reversed(by_distance):
            here = who == around[k]
            for n in range(3):
                picked[n] = jnp.where(here, lane_gather(tables(k, n), lane), picked[n])
        return [
            jnp.where(use > 0, jnp.where(axis == float(n), 0.0, wall_ratio * picked[n]), u[n])
            for n in range(3)
        ]

    def base_of(rho, u):
        return rho - 1.5 * rho * (u[0] * u[0] + u[1] * u[1] + u[2] * u[2])

    for k in range(1, n_gy):
        received(1, k)
    for x in range(2):
        rho = fields[0, x]
        u = wall_velocity(
            fields[4, x], fields[5, x], [fields[1 + n, x] for n in range(3)],
            lambda k, n: table(1, 1, k, n), half[1] * 64,
        )
        base = base_of(rho, u)
        for i in range(13, 27):
            along_e = total_of(u, steps[i])
            if along_e is None:
                posts[i, x] = part[i, x] + base
                continue
            linear = 3.0 * rho * along_e
            even = base + 1.5 * along_e * linear
            posts[i, x] = part[i, x] + (even + linear)
            posts[26 - i, x] = part[26 - i, x] + (even - linear)
    for i, (a, b, c) in enumerate(steps):
        for x in range(2):
            if 0 <= x + a <= 1:
                rolled[i, x] = shifted(posts[i, x], b, c)

    def side(n):
        a = 1 - 2 * n
        rho = fields_in[n, 0]
        u = wall_velocity(
            fields_in[n, 4], fields_in[n, 5], [fields_in[n, 1 + k] for k in range(3)],
            lambda k, m: table(2 * n, 1, k, m), half[1] * 64,
        )
        base = base_of(rho, u)
        for s, (b, c) in enumerate((b, c) for b in (-1, 0, 1) for c in (-1, 0, 1)):
            along_e = total_of(u, (a, b, c))
            linear = 3.0 * rho * along_e
            value = part_in[n, s] + (base + linear + 1.5 * along_e * linear)
            rolled[index_of[a, b, c], 1 - n] = shifted(value, b, c)

    for copy in down:
        copy.wait_recv()
    for k in range(n_gy):
        received(2, k)
    side(1)
    for copy in row + up:
        copy.wait_recv()

    flags = [solid_x[0], solid[0], solid[1], solid_x[1]]
    for xx in range(4):
        for b in (-1, 0, 1):
            plane = flags[xx]
            if b:
                m = 0 if b == 1 else 1
                near = 7 if b == 1 else 0
                if xx in (1, 2):
                    edge = row_of(solid_y, (m, xx - 1), near)
                else:
                    edge = row_of(solid_d, (0 if xx == 0 else 1, m), near)
                plane = pltpu.roll(plane, b % 8, 0)
                plane = jnp.where(row_id == (0 if b == 1 else 7), edge, plane)
            for c in (-1, 0, 1):
                blocked[xx, 3 * (b + 1) + c + 1] = shifted(plane, 0, c)

    at = [row_id == s for s in range(8)]

    def gather_rows(entries):
        value = None
        for s, piece in entries:
            value = piece if value is None else jnp.where(at[s], piece, value)
        return value

    def field_row(k):
        entries = []
        for m in range(2):
            entries.append((4 * m, line(rows_d, m * 9 + 3 + k)))
            entries.append((4 * m + 1, line(rows_in, m * 24 + 12 + k)))
            entries.append((4 * m + 2, line(rows_in, m * 24 + 18 + k)))
            entries.append((4 * m + 3, line(rows_d, (2 + m) * 9 + 3 + k)))
        return gather_rows(entries)

    edge_fields = [field_row(k) for k in range(6)]
    edge_part = {}
    for a in (-1, 0, 1):
        for c in (-1, 0, 1):
            entries = []
            for m in range(2):
                base = m * 24 + 4 * (c + 1)
                if a == 0:
                    entries.append((4 * m + 1, line(rows_in, base)))
                    entries.append((4 * m + 2, line(rows_in, base + 1)))
                elif a == 1:
                    entries.append((4 * m, line(rows_d, m * 9 + c + 1)))
                    entries.append((4 * m + 1, line(rows_in, base + 2)))
                else:
                    entries.append((4 * m + 2, line(rows_in, base + 3)))
                    entries.append((4 * m + 3, line(rows_d, (2 + m) * 9 + c + 1)))
            edge_part[a, c] = gather_rows(entries)

    for k in range(n_gy):
        received(0, k)
    side(0)

    lower = row_id < 4
    across = row_id & 3

    def edge_table(k, n):
        value = table(1, 0, k, n)
        value = jnp.where(lower, value, table(1, 2, k, n))
        for g, s in ((2, 3), (0, 0)):
            value = jnp.where(
                across == s, jnp.where(lower, table(g, 0, k, n), table(g, 2, k, n)), value
            )
        return value

    rho = edge_fields[0]
    u = wall_velocity(
        edge_fields[4], edge_fields[5], edge_fields[1:4], edge_table, (1 - par) * 64
    )
    base = base_of(rho, u)
    u = [u[0], jnp.where(lower, u[1], -u[1]), u[2]]
    for s, (a, c) in enumerate((a, c) for a in (-1, 0, 1) for c in (-1, 0, 1)):
        along_e = total_of(u, (a, 1, c))
        linear = 3.0 * rho * along_e
        value = edge_part[a, c] + (base + linear + 1.5 * along_e * linear)
        edges[s] = shifted(value, 0, c)

    for i, (a, b, c) in enumerate(steps):
        for x in range(2):
            xx = x - a
            if 0 <= xx <= 1:
                value = rolled[i, xx]
            else:
                value = rolled[i, 1 if a == 1 else 0]
            if b:
                m = 0 if b == 1 else 1
                edge = row_of(edges, (3 * (a + 1) + c + 1,), 4 * m + xx + 1)
                value = jnp.where(row_id == (0 if b == 1 else 7), edge, value)
            wall = blocked[xx + 1, 3 * (b + 1) + c + 1]
            out[i, x] = jnp.where(wall != 0, posts[26 - i, x], value)

    for copy in sent + up + row + down:
        copy.wait_send()


def local(*args):
    n_gx, n_gy = lax.axis_size("gx"), lax.axis_size("gy")
    hbm = pl.BlockSpec(memory_space=pl.ANY)
    smem = pl.BlockSpec(memory_space=pltpu.SMEM)
    vmem = pltpu.VMEM
    dma = pltpu.SemaphoreType.DMA
    args = [
        a if k == 5 else pltpu.with_memory_space_constraint(a, pltpu.HBM)
        for k, a in enumerate(args)
    ]
    return pl.pallas_call(
        lambda *refs: body(n_gx, n_gy, *refs),
        name="lattice_step",
        out_shape=vmem((27, 2, 8, 128), F32),
        in_specs=[hbm, hbm, hbm, hbm, hbm, smem, hbm, hbm, hbm],
        out_specs=pl.BlockSpec(memory_space=pltpu.VMEM),
        scratch_shapes=[
            pltpu.SMEM((27,), F32),
            vmem((27, 2, 8, 128), F32),
            vmem((2, 8, 128), I32),
            vmem((1, 1, 512), I32),
            vmem((1, 1, 512), I32),
            vmem((1, 1, 512), I32),
            vmem((1, 1, 8, 512), I32),
            vmem((1, 1, 8, 512), F32),
            vmem((27, 2, 8, 128), F32),
            vmem((6, 2, 8, 128), F32),
            vmem((4, 9, 8, 128), I32),
            vmem((15, 1, 128), F32),
            vmem((3 * n_gy * 6, 1, 128), F32),
            vmem((2, 8, 128), I32),
            vmem((2, 2, 8, 128), I32),
            vmem((2, 2, 8, 128), I32),
            vmem((2, 9, 8, 128), F32),
            vmem((2, 6, 8, 128), F32),
            vmem((84, 1, 128), F32),
            vmem((48, 1, 128), F32),
            vmem((36, 1, 128), F32),
            vmem((27, 2, 8, 128), F32),
            vmem((27, 2, 8, 128), F32),
            vmem((9, 8, 128), F32),
            dma((8,)),
            dma((3 * n_gy - 1,)),
            dma((3 * n_gy,)),
            dma((18,)),
            dma((18,)),
        ],
        compiler_params=pltpu.CompilerParams(
            collective_id=0, has_side_effects=True, vmem_limit_bytes=16 << 20
        ),
    )(*args)


def solution(mesh):
    return jax.shard_map(
        local,
        mesh=mesh,
        in_specs=(
            P(None, "gx", "gy", None),
            P(),
            P("gx", "gy", None),
            P("gx", "gy", None),
            P("gx", "gy", None),
            P("gx", "gy"),
            P("gx", "gy", None),
            P("gx", "gy", None, None),
            P("gx", "gy", None, None),
        ),
        out_specs=P(None, "gx", "gy", None),
        check_vma=False,
    )
```

```python
import jax
import jax.numpy as jnp
import numpy as np
from jax import lax
from jax.experimental import pallas as pl
from jax.experimental.pallas import tpu as pltpu
from jax.sharding import PartitionSpec as P

MESH = pl.DeviceIdType.MESH
wall_ratio = (1.0 / 9.0) ** (1.0 / 7.0)
steps = [(a, b, c) for a in (-1, 0, 1) for b in (-1, 0, 1) for c in (-1, 0, 1)]
index_of = {e: i for i, e in enumerate(steps)}
weight = [float(np.prod([2.0 / 3.0 if v == 0 else 1.0 / 6.0 for v in e])) for e in steps]
F32 = jnp.float32
I32 = jnp.int32


def along(values, axis, combine):
    stride = (9, 3, 1)[axis]
    out = list(values)
    for i in range(27):
        if i // stride % 3 == 0:
            out[i], out[i + stride], out[i + 2 * stride] = combine(
                values[i], values[i + stride], values[i + 2 * stride]
            )
    return out


def to_moments(lo, mid, hi):
    both = hi + lo
    return both + mid, hi - lo, both


def from_moments(zero, one, two):
    return two - one, zero - two, two + one


def equilibrium_moments(rho, vel):
    sq = [v * v for v in vel]
    third = 1.0 / 3.0
    out = []
    for powers in [(a, b, c) for a in range(3) for b in range(3) for c in range(3)]:
        odd = [k for k in range(3) if powers[k] == 1]
        even = [k for k in range(3) if powers[k] == 2]
        scale = third ** len(even)
        if len(odd) == 3:
            out.append(None)
        elif len(odd) == 2:
            out.append(rho * (vel[odd[0]] * vel[odd[1]] * scale))
        elif len(odd) == 1:
            out.append(rho * (vel[odd[0]] * scale))
        elif not even:
            out.append(rho)
        else:
            total = sq[even[0]]
            for k in even[1:]:
                total = total + sq[k]
            out.append(rho * (scale + 3.0 * scale * total))
    return out


def shifted(value, b, c):
    if c:
        value = pltpu.roll(value, c % 128, 1)
    if b:
        value = pltpu.roll(value, b % 8, 0)
    return value


def lane_gather(table, index):
    return jnp.take_along_axis(table, index, axis=1, mode="promise_in_bounds")


def row_of(ref, lead, row):
    return jnp.broadcast_to(ref[lead + (slice(row, row + 1), slice(None))], (8, 128))


def line(ref, row):
    return jnp.broadcast_to(ref[row], (8, 128))


def total_of(u, e):
    total = None
    for n in range(3):
        if e[n]:
            term = u[n] if e[n] > 0 else -u[n]
            total = term if total is None else total + term
    return total


def body(
    n_gx,
    n_gy,
    pop_h,
    relax_h,
    solid_h,
    cell_h,
    normal_h,
    count_s,
    ref_h,
    corner_h,
    cweight_h,
    out,
    relax_s,
    pop,
    solid,
    cell,
    normal,
    sref,
    corner,
    cweight,
    part,
    fields,
    blocked,
    sample,
    sample_in,
    solid_x,
    solid_y,
    solid_d,
    part_in,
    fields_in,
    rows,
    rows_in,
    rows_d,
    rolled,
    posts,
    edges,
    in_sem,
    tally,
    s_send,
    s_recv,
    h_send,
    h_recv,
    ready,
):
    p = lax.axis_index("gx")
    q = lax.axis_index("gy")
    px = [lax.rem(p + n_gx + a, n_gx) for a in (-1, 0, 1)]
    qy = [lax.rem(q + n_gy + b, n_gy) for b in (-1, 0, 1)]
    around = [lax.rem(q + k, n_gy) for k in range(n_gy)]

    loads = [
        pltpu.make_async_copy(src, dst, in_sem.at[k])
        for k, (src, dst) in enumerate(
            [
                (pop_h, pop),
                (corner_h, corner),
                (cweight_h, cweight),
                (relax_h, relax_s),
                (cell_h, cell),
                (normal_h, normal),
                (ref_h, sref),
                (solid_h, solid),
            ]
        )
    ]
    for copy in loads:
        copy.start()

    barrier = pltpu.get_barrier_semaphore()
    by_distance = sorted(range(n_gy), key=lambda k: -min(k, n_gy - k))
    targets = [(a, k) for a in (1, 0, -1) for k in by_distance if a or k]
    greeted = [(a, k) for a in (-1, 0) for k in by_distance if a or k]
    for a, k in greeted:
        pl.semaphore_signal(
            barrier, inc=1, device_id=(px[a + 1], around[k]), device_id_type=MESH
        )
    row_id = lax.broadcasted_iota(I32, (8, 128), 0)

    vel = []
    for copy in loads[:3]:
        copy.wait()
    for x in range(2):
        f = [pop[i, x] * weight[i] for i in range(27)]
        for axis in (2, 1, 0):
            f = along(f, axis, to_moments)
        rho = f[0]
        inv = 1.0 / rho
        u = [f[9] * inv, f[3] * inv, f[1] * inv]
        vel.append(u)
        fields[0, x] = rho
        for k in range(3):
            fields[k + 1, x] = u[k]
        for m in range(27):
            part[m, x] = f[m]

    for j in range(4):
        total = [jnp.zeros((8, 128), F32) for _ in range(3)]
        lanes = slice(128 * j, 128 * (j + 1))
        for k in range(8):
            where = jnp.broadcast_to(corner[0, 0, k : k + 1, lanes], (8, 128))
            share = jnp.broadcast_to(cweight[0, 0, k : k + 1, lanes], (8, 128))
            lane = where & 127
            mine = jnp.where((where >> 7) & 7 == row_id, share, 0.0)
            upper = where >= 1024
            for n in range(3):
                got = jnp.where(upper, lane_gather(vel[1][n], lane), lane_gather(vel[0][n], lane))
                total[n] = total[n] + mine * got
        for n in range(3):
            summed = jnp.sum(total[n], axis=0, keepdims=True)
            sample[3 * j + n] = summed
            if j == 0:
                sample[12 + n] = summed

    par = lax.rem(q, 2)

    def window(d):
        return 3 * lax.div(lax.rem(d + n_gy - 1, n_gy), 2)

    mine = window(q)
    for r in range(6):
        sample_in[(n_gy + q) * 6 + r] = sample[mine + r]

    def send(src, dst, send_sem, recv_sem, peer):
        pltpu.make_async_remote_copy(
            src_ref=src, dst_ref=dst, send_sem=send_sem, recv_sem=recv_sem,
            device_id=peer, device_id_type=MESH,
        ).start()

    def send_samples(a):
        for b, k in targets:
            if b == a:
                send(
                    sample.at[pl.ds(window(around[k]), 6)],
                    sample_in.at[pl.ds(((1 - a) * n_gy + q) * 6, 6)],
                    s_send,
                    s_recv.at[1 - a],
                    (px[a + 1], around[k]),
                )

    def send_side(n):
        a = 1 - 2 * n
        x = 1 - n
        to = px[a + 1]
        halo = []
        for m, b in enumerate((1, -1)):
            halo.append(
                (rows.at[pl.ds(42 * m + 24 + 9 * n, 9)], rows_d.at[pl.ds((2 * n + m) * 9, 9)], (to, qy[b + 1]))
            )
        halo.append((fields.at[:, x], fields_in.at[n], (to, q)))
        halo.append((part.at[pl.ds(18 - 18 * n, 9), x], part_in.at[n], (to, q)))
        halo.append((solid.at[x], solid_x.at[n], (to, q)))
        for m, b in enumerate((1, -1)):
            halo.append((solid.at[x], solid_d.at[n, m], (to, qy[b + 1])))
        for src, dst, peer in halo:
            send(src, dst, h_send, h_recv.at[n], peer)

    def send_row():
        for m, b in enumerate((1, -1)):
            to = (p, qy[b + 1])
            send(rows.at[pl.ds(42 * m, 24)], rows_in.at[pl.ds(24 * m, 24)], h_send, h_recv.at[2], to)
            send(solid, solid_y.at[m], h_send, h_recv.at[2], to)

    def arrived(sem, lines):
        span = tally.at[pl.ds(0, lines)]
        pltpu.make_async_copy(span, span, sem).wait()

    side_lines = 2 * 9 + 48 + 72 + 24
    row_lines = 2 * (24 + 16)

    pl.semaphore_wait(barrier, len(greeted))
    send_samples(1)
    for k in by_distance:
        pl.semaphore_signal(
            ready, inc=1, device_id=(px[2], around[k]), device_id_type=MESH
        )

    for copy in loads[4:]:
        copy.wait()
    cells = cell[0]
    live = lax.broadcasted_iota(I32, (1, 512), 1) < count_s[0, 0]
    refs = sref[0]
    first = jnp.where(live, (refs & 63) + 1, 0)
    second = jnp.where(live, (refs >> 6) * 8 + normal[0], 0)
    rows16 = lax.broadcasted_iota(I32, (16, 512), 0) == (cells >> 7)
    left = jnp.concatenate(
        [jnp.where(rows16, first, 0), jnp.where(rows16, second, 0)], axis=0
    ).astype(F32).astype(jnp.bfloat16)
    right = jnp.where(
        lax.broadcasted_iota(I32, (128, 512), 0) == (cells & 127), 1.0, 0.0
    ).astype(jnp.bfloat16)
    code = lax.dot_general(
        left, right, (((1,), (1,)), ((), ())), preferred_element_type=F32
    ).astype(I32)
    slot = code[0:16]
    owner = code[16:32]
    use = jnp.where(slot > 0, (owner >> 3) * 64 + slot, 0).astype(F32)
    axes = ((owner & 7) >> 1).astype(F32)
    for x in range(2):
        fields[4, x] = use[8 * x : 8 * x + 8]
        fields[5, x] = axes[8 * x : 8 * x + 8]

    loads[3].wait()
    for x in range(2):
        f = [part[m, x] for m in range(27)]
        balance = equilibrium_moments(fields[0, x], [fields[1 + k, x] for k in range(3)])
        for m in range(27):
            off = f[m] if balance[m] is None else f[m] - balance[m]
            f[m] = off * (1.0 - relax_s[m])
        for axis in (2, 1, 0):
            f = along(f, axis, from_moments)
        for i, e in enumerate(steps):
            part[i, x] = f[i] * float(np.prod([1.5 if v == 0 else 3.0 for v in e]))

    for m, b in enumerate((1, -1)):
        near = slice(7, 8) if b == 1 else slice(0, 1)
        base = 42 * m
        for c in (-1, 0, 1):
            for s, (a, x) in enumerate(((0, 0), (0, 1), (1, 0), (-1, 1))):
                rows[base + 4 * (c + 1) + s] = part[index_of[a, b, c], x, near]
            for n, (a, x) in enumerate(((1, 1), (-1, 0))):
                rows[base + 24 + 9 * n + c + 1] = part[index_of[a, b, c], x, near]
        for k in range(6):
            for x in range(2):
                value = fields[k, x, near]
                rows[base + 12 + 6 * x + k] = value
                rows[base + 27 + 9 * (1 - x) + k] = value

    send_side(0)
    send_samples(0)
    send_row()
    pl.semaphore_wait(ready, n_gy)
    send_samples(-1)
    send_side(1)

    chunk = [0, 1 - par, 1]
    half = [1 - par, par, 1 - par]

    def table(g, t, k, n):
        return line(sample_in, (g * n_gy + around[k]) * 6 + 3 * chunk[t] + n)

    def wall_velocity(use, axis, u, tables, lanes):
        use = use.astype(I32)
        spot = use - 1
        who = spot >> 6
        lane = (spot & 63) + lanes
        picked = [jnp.zeros((8, 128), F32) for _ in range(3)]
        for k in reversed(by_distance):
            here = who == around[k]
            for n in range(3):
                picked[n] = jnp.where(here, lane_gather(tables(k, n), lane), picked[n])
        return [
            jnp.where(use > 0, jnp.where(axis == float(n), 0.0, wall_ratio * picked[n]), u[n])
            for n in range(3)
        ]

    def base_of(rho, u):
        return rho - 1.5 * rho * (u[0] * u[0] + u[1] * u[1] + u[2] * u[2])

    arrived(s_recv.at[1], (n_gy - 1) * 6)
    for x in range(2):
        rho = fields[0, x]
        u = wall_velocity(
            fields[4, x], fields[5, x], [fields[1 + n, x] for n in range(3)],
            lambda k, n: table(1, 1, k, n), half[1] * 64,
        )
        base = base_of(rho, u)
        for i in range(13, 27):
            along_e = total_of(u, steps[i])
            if along_e is None:
                posts[i, x] = part[i, x] + base
                continue
            linear = 3.0 * rho * along_e
            even = base + 1.5 * along_e * linear
            posts[i, x] = part[i, x] + (even + linear)
            posts[26 - i, x] = part[26 - i, x] + (even - linear)
    for i, (a, b, c) in enumerate(steps):
        for x in range(2):
            if 0 <= x + a <= 1:
                rolled[i, x] = shifted(posts[i, x], b, c)

    def side(n):
        a = 1 - 2 * n
        rho = fields_in[n, 0]
        u = wall_velocity(
            fields_in[n, 4], fields_in[n, 5], [fields_in[n, 1 + k] for k in range(3)],
            lambda k, m: table(2 * n, 1, k, m), half[1] * 64,
        )
        base = base_of(rho, u)
        for s, (b, c) in enumerate((b, c) for b in (-1, 0, 1) for c in (-1, 0, 1)):
            along_e = total_of(u, (a, b, c))
            linear = 3.0 * rho * along_e
            value = part_in[n, s] + (base + linear + 1.5 * along_e * linear)
            rolled[index_of[a, b, c], 1 - n] = shifted(value, b, c)

    def block_plane(xx, plane):
        for b in (-1, 0, 1):
            moved = plane
            if b:
                m = 0 if b == 1 else 1
                near = 7 if b == 1 else 0
                if xx in (1, 2):
                    edge = row_of(solid_y, (m, xx - 1), near)
                else:
                    edge = row_of(solid_d, (0 if xx == 0 else 1, m), near)
                moved = pltpu.roll(plane, b % 8, 0)
                moved = jnp.where(row_id == (0 if b == 1 else 7), edge, moved)
            for c in (-1, 0, 1):
                blocked[xx, 3 * (b + 1) + c + 1] = shifted(moved, 0, c)

    at = [row_id == s for s in range(8)]
    lower = row_id < 4
    across = row_id & 3

    def gather_rows(entries):
        value = None
        for s, piece in entries:
            value = piece if value is None else jnp.where(at[s], piece, value)
        return value

    def field_row(k, near):
        entries = []
        for m in range(2):
            if near:
                entries.append((4 * m + 1, line(rows_in, m * 24 + 12 + k)))
                entries.append((4 * m + 2, line(rows_in, m * 24 + 18 + k)))
                entries.append((4 * m + 3, line(rows_d, (2 + m) * 9 + 3 + k)))
            else:
                entries.append((4 * m, line(rows_d, m * 9 + 3 + k)))
        return gather_rows(entries)

    def part_row(a, c, near):
        entries = []
        for m in range(2):
            base = m * 24 + 4 * (c + 1)
            if not near:
                entries.append((4 * m, line(rows_d, m * 9 + c + 1)))
            elif a == 0:
                entries.append((4 * m + 1, line(rows_in, base)))
                entries.append((4 * m + 2, line(rows_in, base + 1)))
            elif a == 1:
                entries.append((4 * m + 1, line(rows_in, base + 2)))
            else:
                entries.append((4 * m + 2, line(rows_in, base + 3)))
                entries.append((4 * m + 3, line(rows_d, (2 + m) * 9 + c + 1)))
        return gather_rows(entries)

    def table_near(k, n):
        value = jnp.where(lower, table(1, 0, k, n), table(1, 2, k, n))
        other = jnp.where(lower, table(2, 0, k, n), table(2, 2, k, n))
        return jnp.where(across == 3, other, value)

    def table_far(k, n):
        return jnp.where(lower, table(0, 0, k, n), table(0, 2, k, n))

    def edge_rows(found, parts, tables, where):
        rho = found[0]
        u = wall_velocity(found[4], found[5], found[1:4], tables, (1 - par) * 64)
        base = base_of(rho, u)
        u = [u[0], jnp.where(lower, u[1], -u[1]), u[2]]
        for (a, c), piece in parts.items():
            along_e = total_of(u, (a, 1, c))
            linear = 3.0 * rho * along_e
            value = piece + (base + linear + 1.5 * along_e * linear)
            edges[where + 3 * (a + 1) + c + 1] = shifted(value, 0, c)

    def finish(far):
        for i, (a, b, c) in enumerate(steps):
            for x in range(2):
                xx = x - a
                if (xx == -1) != far:
                    continue
                value = rolled[i, xx if 0 <= xx <= 1 else 1 if a == 1 else 0]
                if b:
                    m = 0 if b == 1 else 1
                    s = (9 if far else 0) + 3 * (a + 1) + c + 1
                    edge = row_of(edges, (s,), 4 * m + xx + 1)
                    value = jnp.where(row_id == (0 if b == 1 else 7), edge, value)
                wall = blocked[xx + 1, 3 * (b + 1) + c + 1]
                out[i, x] = jnp.where(wall != 0, posts[26 - i, x], value)

    arrived(h_recv.at[2], row_lines)
    arrived(h_recv.at[1], side_lines)
    for xx, plane in ((1, solid[0]), (2, solid[1]), (3, solid_x[1])):
        block_plane(xx, plane)
    found = [field_row(k, True) for k in range(6)]
    parts = {(a, c): part_row(a, c, True) for a in (-1, 0, 1) for c in (-1, 0, 1)}
    arrived(s_recv.at[2], n_gy * 6)
    side(1)
    edge_rows(found, parts, table_near, 0)
    finish(False)

    arrived(h_recv.at[0], side_lines)
    block_plane(0, solid_x[0])
    found = [field_row(k, False) for k in range(6)]
    parts = {(1, c): part_row(1, c, False) for c in (-1, 0, 1)}
    arrived(s_recv.at[0], n_gy * 6)
    side(0)
    edge_rows(found, parts, table_far, 9)
    finish(True)

    arrived(s_send, len(targets) * 6)
    arrived(h_send, 2 * side_lines + row_lines)


def local(*args):
    n_gx, n_gy = lax.axis_size("gx"), lax.axis_size("gy")
    hbm = pl.BlockSpec(memory_space=pl.ANY)
    smem = pl.BlockSpec(memory_space=pltpu.SMEM)
    vmem = pltpu.VMEM
    dma = pltpu.SemaphoreType.DMA
    args = [
        a if k == 5 else pltpu.with_memory_space_constraint(a, pltpu.HBM)
        for k, a in enumerate(args)
    ]
    return pl.pallas_call(
        lambda *refs: body(n_gx, n_gy, *refs),
        name="lattice_step",
        out_shape=vmem((27, 2, 8, 128), F32),
        in_specs=[hbm, hbm, hbm, hbm, hbm, smem, hbm, hbm, hbm],
        out_specs=pl.BlockSpec(memory_space=pltpu.VMEM),
        scratch_shapes=[
            pltpu.SMEM((27,), F32),
            vmem((27, 2, 8, 128), F32),
            vmem((2, 8, 128), I32),
            vmem((1, 1, 512), I32),
            vmem((1, 1, 512), I32),
            vmem((1, 1, 512), I32),
            vmem((1, 1, 8, 512), I32),
            vmem((1, 1, 8, 512), F32),
            vmem((27, 2, 8, 128), F32),
            vmem((6, 2, 8, 128), F32),
            vmem((4, 9, 8, 128), I32),
            vmem((15, 1, 128), F32),
            vmem((3 * n_gy * 6, 1, 128), F32),
            vmem((2, 8, 128), I32),
            vmem((2, 2, 8, 128), I32),
            vmem((2, 2, 8, 128), I32),
            vmem((2, 9, 8, 128), F32),
            vmem((2, 6, 8, 128), F32),
            vmem((84, 1, 128), F32),
            vmem((48, 1, 128), F32),
            vmem((36, 1, 128), F32),
            vmem((27, 2, 8, 128), F32),
            vmem((27, 2, 8, 128), F32),
            vmem((18, 8, 128), F32),
            dma((8,)),
            vmem((404, 1, 128), F32),
            dma(()),
            dma((3,)),
            dma(()),
            dma((3,)),
            pltpu.SemaphoreType.REGULAR,
        ],
        compiler_params=pltpu.CompilerParams(
            collective_id=0, has_side_effects=True, vmem_limit_bytes=16 << 20
        ),
    )(*args)


def solution(mesh):
    return jax.shard_map(
        local,
        mesh=mesh,
        in_specs=(
            P(None, "gx", "gy", None),
            P(),
            P("gx", "gy", None),
            P("gx", "gy", None),
            P("gx", "gy", None),
            P("gx", "gy"),
            P("gx", "gy", None),
            P("gx", "gy", None, None),
            P("gx", "gy", None, None),
        ),
        out_specs=P(None, "gx", "gy", None),
        check_vma=False,
    )
```

```python
import jax
import jax.numpy as jnp
import numpy as np
from jax import lax
from jax.experimental import pallas as pl
from jax.experimental.pallas import tpu as pltpu
from jax.sharding import PartitionSpec as P

MESH = pl.DeviceIdType.MESH
wall_ratio = (1.0 / 9.0) ** (1.0 / 7.0)
steps = [(a, b, c) for a in (-1, 0, 1) for b in (-1, 0, 1) for c in (-1, 0, 1)]
index_of = {e: i for i, e in enumerate(steps)}
weight = [float(np.prod([2.0 / 3.0 if v == 0 else 1.0 / 6.0 for v in e])) for e in steps]
F32 = jnp.float32
I32 = jnp.int32


def along(values, axis, combine):
    stride = (9, 3, 1)[axis]
    out = list(values)
    for i in range(27):
        if i // stride % 3 == 0:
            out[i], out[i + stride], out[i + 2 * stride] = combine(
                values[i], values[i + stride], values[i + 2 * stride]
            )
    return out


def to_moments(lo, mid, hi):
    both = hi + lo
    return both + mid, hi - lo, both


def from_moments(zero, one, two):
    return two - one, zero - two, two + one


def equilibrium_moments(rho, vel):
    sq = [v * v for v in vel]
    third = 1.0 / 3.0
    out = []
    for powers in [(a, b, c) for a in range(3) for b in range(3) for c in range(3)]:
        odd = [k for k in range(3) if powers[k] == 1]
        even = [k for k in range(3) if powers[k] == 2]
        scale = third ** len(even)
        if len(odd) == 3:
            out.append(None)
        elif len(odd) == 2:
            out.append(rho * (vel[odd[0]] * vel[odd[1]] * scale))
        elif len(odd) == 1:
            out.append(rho * (vel[odd[0]] * scale))
        elif not even:
            out.append(rho)
        else:
            total = sq[even[0]]
            for k in even[1:]:
                total = total + sq[k]
            out.append(rho * (scale + 3.0 * scale * total))
    return out


def shifted(value, b, c):
    if c:
        value = pltpu.roll(value, c % 128, 1)
    if b:
        value = pltpu.roll(value, b % 8, 0)
    return value


def lane_gather(table, index):
    return jnp.take_along_axis(table, index, axis=1, mode="promise_in_bounds")


def row_of(ref, lead, row):
    return jnp.broadcast_to(ref[lead + (slice(row, row + 1), slice(None))], (8, 128))


def line(ref, row):
    return jnp.broadcast_to(ref[row], (8, 128))


def total_of(u, e):
    total = None
    for n in range(3):
        if e[n]:
            term = u[n] if e[n] > 0 else -u[n]
            total = term if total is None else total + term
    return total


def body(
    n_gx,
    n_gy,
    pop_h,
    relax_h,
    solid_h,
    cell_h,
    normal_h,
    count_s,
    ref_h,
    corner_h,
    cweight_h,
    out,
    relax_s,
    pop,
    solid,
    cell,
    normal,
    sref,
    corner,
    cweight,
    part,
    fields,
    blocked,
    sample,
    sample_in,
    solid_x,
    solid_y,
    solid_d,
    part_in,
    fields_in,
    rows,
    rows_in,
    rows_d,
    rolled,
    posts,
    edges,
    in_sem,
    tally,
    s_send,
    s_recv,
    h_send,
    h_recv,
    ready,
    whole,
):
    p = lax.axis_index("gx")
    pop = pop_h
    corner = corner_h
    cweight = cweight_h
    q = lax.axis_index("gy")
    px = [lax.rem(p + n_gx + a, n_gx) for a in (-1, 0, 1)]
    qy = [lax.rem(q + n_gy + b, n_gy) for b in (-1, 0, 1)]
    around = [lax.rem(q + k, n_gy) for k in range(n_gy)]

    loads = [
        pltpu.make_async_copy(src, dst, in_sem.at[k])
        for k, (src, dst) in enumerate(
            [
                (relax_h, relax_s),
                (cell_h, cell),
                (normal_h, normal),
                (ref_h, sref),
                (solid_h, solid),
            ]
        )
    ]
    for copy in loads:
        copy.start()

    barrier = pltpu.get_barrier_semaphore()
    by_distance = sorted(range(n_gy), key=lambda k: -min(k, n_gy - k))
    targets = [(a, k) for a in (1, 0, -1) for k in by_distance if a or k]
    for k in by_distance:
        pl.semaphore_signal(
            barrier, inc=1, device_id=(px[0], around[k]), device_id_type=MESH
        )
    row_id = lax.broadcasted_iota(I32, (8, 128), 0)

    vel = []
    for copy in loads[:0]:
        copy.wait()
    for x in range(2):
        f = [pop[i, x] * weight[i] for i in range(27)]
        for axis in (2, 1, 0):
            f = along(f, axis, to_moments)
        rho = f[0]
        inv = 1.0 / rho
        u = [f[9] * inv, f[3] * inv, f[1] * inv]
        vel.append(u)
        fields[0, x] = rho
        for k in range(3):
            fields[k + 1, x] = u[k]
        for m in range(27):
            part[m, x] = f[m]

    for j in range(4):
        total = [jnp.zeros((8, 128), F32) for _ in range(3)]
        lanes = slice(128 * j, 128 * (j + 1))
        for k in range(8):
            where = jnp.broadcast_to(corner[0, 0, k : k + 1, lanes], (8, 128))
            share = jnp.broadcast_to(cweight[0, 0, k : k + 1, lanes], (8, 128))
            lane = where & 127
            mine = jnp.where((where >> 7) & 7 == row_id, share, 0.0)
            upper = where >= 1024
            for n in range(3):
                got = jnp.where(upper, lane_gather(vel[1][n], lane), lane_gather(vel[0][n], lane))
                total[n] = total[n] + mine * got
        for n in range(3):
            summed = jnp.sum(total[n], axis=0, keepdims=True)
            sample[3 * j + n] = summed
            if j == 0:
                sample[12 + n] = summed

    par = lax.rem(q, 2)

    def window(d):
        return 3 * lax.div(lax.rem(d + n_gy - 1, n_gy), 2)

    mine = window(q)
    for r in range(6):
        sample_in[(n_gy + q) * 6 + r] = sample[mine + r]

    def send(src, dst, send_sem, recv_sem, peer):
        pltpu.make_async_remote_copy(
            src_ref=src, dst_ref=dst, send_sem=send_sem, recv_sem=recv_sem,
            device_id=peer, device_id_type=MESH,
        ).start()

    def send_samples(a):
        for b, k in targets:
            if b == a:
                send(
                    sample.at[pl.ds(window(around[k]), 6)],
                    sample_in.at[pl.ds(((1 - a) * n_gy + q) * 6, 6)],
                    s_send,
                    s_recv.at[1 - a],
                    (px[a + 1], around[k]),
                )

    def send_side(n):
        a = 1 - 2 * n
        x = 1 - n
        to = px[a + 1]
        halo = []
        for m, b in enumerate((1, -1)):
            halo.append(
                (rows.at[pl.ds(42 * m + 24 + 9 * n, 9)], rows_d.at[pl.ds((2 * n + m) * 9, 9)], (to, qy[b + 1]))
            )
        halo.append((fields.at[:, x], fields_in.at[n], (to, q)))
        halo.append((part.at[pl.ds(18 - 18 * n, 9), x], part_in.at[n], (to, q)))
        halo.append((solid.at[x], solid_x.at[n], (to, q)))
        for m, b in enumerate((1, -1)):
            halo.append((solid.at[x], solid_d.at[n, m], (to, qy[b + 1])))
        for src, dst, peer in halo:
            send(src, dst, h_send, h_recv.at[n], peer)

    def send_row():
        for m, b in enumerate((1, -1)):
            to = (p, qy[b + 1])
            send(rows.at[pl.ds(42 * m, 24)], rows_in.at[pl.ds(24 * m, 24)], h_send, h_recv.at[2], to)
            send(solid, solid_y.at[m], h_send, h_recv.at[2], to)

    def arrived(sem, lines):
        span = tally.at[pl.ds(0, lines)]
        pltpu.make_async_copy(span, span, sem).wait()

    side_lines = 2 * 9 + 48 + 72 + 24
    row_lines = 2 * (24 + 16)

    pl.semaphore_wait(barrier, n_gy)
    send_samples(1)
    for k in by_distance:
        pl.semaphore_signal(
            ready, inc=1, device_id=(px[2], around[k]), device_id_type=MESH
        )

    for copy in loads[1:]:
        copy.wait()
    cells = cell[0]
    live = count_s[...] > 0
    refs = sref[0]
    first = jnp.where(live, (refs & 63) + 1, 0)
    second = jnp.where(live, (refs >> 6) * 8 + normal[0], 0)
    rows16 = lax.broadcasted_iota(I32, (16, 512), 0) == (cells >> 7)
    left = jnp.concatenate(
        [jnp.where(rows16, first, 0), jnp.where(rows16, second, 0)], axis=0
    ).astype(F32).astype(jnp.bfloat16)
    right = jnp.where(
        lax.broadcasted_iota(I32, (128, 512), 0) == (cells & 127), 1.0, 0.0
    ).astype(jnp.bfloat16)
    code = lax.dot_general(
        left, right, (((1,), (1,)), ((), ())), preferred_element_type=F32
    ).astype(I32)
    slot = code[0:16]
    owner = code[16:32]
    use = jnp.where(slot > 0, (owner >> 3) * 64 + slot, 0).astype(F32)
    axes = ((owner & 7) >> 1).astype(F32)
    for x in range(2):
        fields[4, x] = use[8 * x : 8 * x + 8]
        fields[5, x] = axes[8 * x : 8 * x + 8]

    loads[0].wait()
    for x in range(2):
        f = [part[m, x] for m in range(27)]
        balance = equilibrium_moments(fields[0, x], [fields[1 + k, x] for k in range(3)])
        for m in range(27):
            off = f[m] if balance[m] is None else f[m] - balance[m]
            f[m] = off * (1.0 - relax_s[m])
        for axis in (2, 1, 0):
            f = along(f, axis, from_moments)
        for i, e in enumerate(steps):
            part[i, x] = f[i] * float(np.prod([1.5 if v == 0 else 3.0 for v in e]))

    for m, b in enumerate((1, -1)):
        near = slice(7, 8) if b == 1 else slice(0, 1)
        base = 42 * m
        for c in (-1, 0, 1):
            for s, (a, x) in enumerate(((0, 0), (0, 1), (1, 0), (-1, 1))):
                rows[base + 4 * (c + 1) + s] = part[index_of[a, b, c], x, near]
            for n, (a, x) in enumerate(((1, 1), (-1, 0))):
                rows[base + 24 + 9 * n + c + 1] = part[index_of[a, b, c], x, near]
        for k in range(6):
            for x in range(2):
                value = fields[k, x, near]
                rows[base + 12 + 6 * x + k] = value
                rows[base + 27 + 9 * (1 - x) + k] = value

    send_side(0)
    def greet():
        pl.semaphore_wait(ready, n_gy)
        pl.semaphore_signal(whole, inc=1, device_id=(px[0], q), device_id_type=MESH)

    pl.when(p != 0)(greet)
    pl.semaphore_wait(whole, 1)
    send_samples(0)
    send_row()
    pl.when(p == 0)(greet)
    send_samples(-1)
    send_side(1)

    chunk = [0, 1 - par, 1]
    half = [1 - par, par, 1 - par]

    def table(g, t, k, n):
        return line(sample_in, (g * n_gy + around[k]) * 6 + 3 * chunk[t] + n)

    def wall_velocity(use, axis, u, tables, lanes):
        use = use.astype(I32)
        spot = use - 1
        who = spot >> 6
        lane = (spot & 63) + lanes
        picked = [jnp.zeros((8, 128), F32) for _ in range(3)]
        for k in reversed(by_distance):
            here = who == around[k]
            for n in range(3):
                picked[n] = jnp.where(here, lane_gather(tables(k, n), lane), picked[n])
        return [
            jnp.where(use > 0, jnp.where(axis == float(n), 0.0, wall_ratio * picked[n]), u[n])
            for n in range(3)
        ]

    def base_of(rho, u):
        return rho - 1.5 * rho * (u[0] * u[0] + u[1] * u[1] + u[2] * u[2])

    arrived(s_recv.at[1], (n_gy - 1) * 6)
    for x in range(2):
        rho = fields[0, x]
        u = wall_velocity(
            fields[4, x], fields[5, x], [fields[1 + n, x] for n in range(3)],
            lambda k, n: table(1, 1, k, n), half[1] * 64,
        )
        base = base_of(rho, u)
        for i in range(13, 27):
            along_e = total_of(u, steps[i])
            if along_e is None:
                posts[i, x] = part[i, x] + base
                continue
            linear = 3.0 * rho * along_e
            even = base + 1.5 * along_e * linear
            posts[i, x] = part[i, x] + (even + linear)
            posts[26 - i, x] = part[26 - i, x] + (even - linear)
    for i, (a, b, c) in enumerate(steps):
        for x in range(2):
            if 0 <= x + a <= 1:
                rolled[i, x] = shifted(posts[i, x], b, c)

    def side(n):
        a = 1 - 2 * n
        rho = fields_in[n, 0]
        u = wall_velocity(
            fields_in[n, 4], fields_in[n, 5], [fields_in[n, 1 + k] for k in range(3)],
            lambda k, m: table(2 * n, 1, k, m), half[1] * 64,
        )
        base = base_of(rho, u)
        for s, (b, c) in enumerate((b, c) for b in (-1, 0, 1) for c in (-1, 0, 1)):
            along_e = total_of(u, (a, b, c))
            linear = 3.0 * rho * along_e
            value = part_in[n, s] + (base + linear + 1.5 * along_e * linear)
            rolled[index_of[a, b, c], 1 - n] = shifted(value, b, c)

    def block_plane(xx, plane):
        for b in (-1, 0, 1):
            moved = plane
            if b:
                m = 0 if b == 1 else 1
                near = 7 if b == 1 else 0
                if xx in (1, 2):
                    edge = row_of(solid_y, (m, xx - 1), near)
                else:
                    edge = row_of(solid_d, (0 if xx == 0 else 1, m), near)
                moved = pltpu.roll(plane, b % 8, 0)
                moved = jnp.where(row_id == (0 if b == 1 else 7), edge, moved)
            for c in (-1, 0, 1):
                blocked[xx, 3 * (b + 1) + c + 1] = shifted(moved, 0, c)

    at = [row_id == s for s in range(8)]
    lower = row_id < 4
    across = row_id & 3

    def gather_rows(entries):
        value = None
        for s, piece in entries:
            value = piece if value is None else jnp.where(at[s], piece, value)
        return value

    def field_row(k, near):
        entries = []
        for m in range(2):
            if near:
                entries.append((4 * m + 1, line(rows_in, m * 24 + 12 + k)))
                entries.append((4 * m + 2, line(rows_in, m * 24 + 18 + k)))
                entries.append((4 * m + 3, line(rows_d, (2 + m) * 9 + 3 + k)))
            else:
                entries.append((4 * m, line(rows_d, m * 9 + 3 + k)))
        return gather_rows(entries)

    def part_row(a, c, near):
        entries = []
        for m in range(2):
            base = m * 24 + 4 * (c + 1)
            if not near:
                entries.append((4 * m, line(rows_d, m * 9 + c + 1)))
            elif a == 0:
                entries.append((4 * m + 1, line(rows_in, base)))
                entries.append((4 * m + 2, line(rows_in, base + 1)))
            elif a == 1:
                entries.append((4 * m + 1, line(rows_in, base + 2)))
            else:
                entries.append((4 * m + 2, line(rows_in, base + 3)))
                entries.append((4 * m + 3, line(rows_d, (2 + m) * 9 + c + 1)))
        return gather_rows(entries)

    def table_near(k, n):
        value = jnp.where(lower, table(1, 0, k, n), table(1, 2, k, n))
        other = jnp.where(lower, table(2, 0, k, n), table(2, 2, k, n))
        return jnp.where(across == 3, other, value)

    def table_far(k, n):
        return jnp.where(lower, table(0, 0, k, n), table(0, 2, k, n))

    def edge_rows(found, parts, tables, where):
        rho = found[0]
        u = wall_velocity(found[4], found[5], found[1:4], tables, (1 - par) * 64)
        base = base_of(rho, u)
        u = [u[0], jnp.where(lower, u[1], -u[1]), u[2]]
        for (a, c), piece in parts.items():
            along_e = total_of(u, (a, 1, c))
            linear = 3.0 * rho * along_e
            value = piece + (base + linear + 1.5 * along_e * linear)
            edges[where + 3 * (a + 1) + c + 1] = shifted(value, 0, c)

    def finish(far):
        for i, (a, b, c) in enumerate(steps):
            for x in range(2):
                xx = x - a
                if (xx == -1) != far:
                    continue
                value = rolled[i, xx if 0 <= xx <= 1 else 1 if a == 1 else 0]
                if b:
                    m = 0 if b == 1 else 1
                    s = (9 if far else 0) + 3 * (a + 1) + c + 1
                    edge = row_of(edges, (s,), 4 * m + xx + 1)
                    value = jnp.where(row_id == (0 if b == 1 else 7), edge, value)
                wall = blocked[xx + 1, 3 * (b + 1) + c + 1]
                out[i, x] = jnp.where(wall != 0, posts[26 - i, x], value)

    arrived(h_recv.at[2], row_lines)
    arrived(h_recv.at[1], side_lines)
    for xx, plane in ((1, solid[0]), (2, solid[1]), (3, solid_x[1])):
        block_plane(xx, plane)
    found = [field_row(k, True) for k in range(6)]
    parts = {(a, c): part_row(a, c, True) for a in (-1, 0, 1) for c in (-1, 0, 1)}
    arrived(s_recv.at[2], n_gy * 6)
    side(1)
    edge_rows(found, parts, table_near, 0)
    finish(False)

    arrived(h_recv.at[0], side_lines)
    block_plane(0, solid_x[0])
    found = [field_row(k, False) for k in range(6)]
    parts = {(1, c): part_row(1, c, False) for c in (-1, 0, 1)}
    arrived(s_recv.at[0], n_gy * 6)
    side(0)
    edge_rows(found, parts, table_far, 9)
    finish(True)

    arrived(s_send, len(targets) * 6)
    arrived(h_send, 2 * side_lines + row_lines)


def mark_live(count, live):
    spot = lax.broadcasted_iota(I32, live.shape, 1)
    live[...] = jnp.where(spot < count[0, 0], 1, 0)


def local(*args):
    n_gx, n_gy = lax.axis_size("gx"), lax.axis_size("gy")
    hbm = pl.BlockSpec(memory_space=pl.ANY)
    smem = pl.BlockSpec(memory_space=pltpu.SMEM)
    vmem = pltpu.VMEM
    dma = pltpu.SemaphoreType.DMA
    args = [
        a if k in (0, 5, 7, 8) else pltpu.with_memory_space_constraint(a, pltpu.HBM)
        for k, a in enumerate(args)
    ]
    args[5] = pl.pallas_call(
        mark_live,
        name="mark_live",
        out_shape=vmem((1, 512), I32),
        in_specs=[smem],
        out_specs=pl.BlockSpec(memory_space=pltpu.VMEM),
        cost_estimate=pl.CostEstimate(flops=100000000, bytes_accessed=1000, transcendentals=0),
    )(args[5])
    return pl.pallas_call(
        lambda *refs: body(n_gx, n_gy, *refs),
        name="lattice_step",
        out_shape=vmem((27, 2, 8, 128), F32),
        in_specs=[pl.BlockSpec(memory_space=pltpu.VMEM), hbm, hbm, hbm, hbm, pl.BlockSpec(memory_space=pltpu.VMEM), hbm, pl.BlockSpec(memory_space=pltpu.VMEM), pl.BlockSpec(memory_space=pltpu.VMEM)],
        out_specs=pl.BlockSpec(memory_space=pltpu.VMEM),
        scratch_shapes=[
            pltpu.SMEM((27,), F32),
            vmem((27, 2, 8, 128), F32),
            vmem((2, 8, 128), I32),
            vmem((1, 1, 512), I32),
            vmem((1, 1, 512), I32),
            vmem((1, 1, 512), I32),
            vmem((1, 1, 8, 512), I32),
            vmem((1, 1, 8, 512), F32),
            vmem((27, 2, 8, 128), F32),
            vmem((6, 2, 8, 128), F32),
            vmem((4, 9, 8, 128), I32),
            vmem((15, 1, 128), F32),
            vmem((3 * n_gy * 6, 1, 128), F32),
            vmem((2, 8, 128), I32),
            vmem((2, 2, 8, 128), I32),
            vmem((2, 2, 8, 128), I32),
            vmem((2, 9, 8, 128), F32),
            vmem((2, 6, 8, 128), F32),
            vmem((84, 1, 128), F32),
            vmem((48, 1, 128), F32),
            vmem((36, 1, 128), F32),
            vmem((27, 2, 8, 128), F32),
            vmem((27, 2, 8, 128), F32),
            vmem((18, 8, 128), F32),
            dma((8,)),
            vmem((404, 1, 128), F32),
            dma(()),
            dma((3,)),
            dma(()),
            dma((3,)),
            pltpu.SemaphoreType.REGULAR,
            pltpu.SemaphoreType.REGULAR,
        ],
        compiler_params=pltpu.CompilerParams(
            collective_id=0, has_side_effects=True, vmem_limit_bytes=16 << 20
        ),
    )(*args)


def solution(mesh):
    return jax.shard_map(
        local,
        mesh=mesh,
        in_specs=(
            P(None, "gx", "gy", None),
            P(),
            P("gx", "gy", None),
            P("gx", "gy", None),
            P("gx", "gy", None),
            P("gx", "gy"),
            P("gx", "gy", None),
            P("gx", "gy", None, None),
            P("gx", "gy", None, None),
        ),
        out_specs=P(None, "gx", "gy", None),
        check_vma=False,
    )
```

```python
import jax
import jax.numpy as jnp
import numpy as np
from jax import lax
from jax.experimental import pallas as pl
from jax.experimental.pallas import tpu as pltpu
from jax.sharding import PartitionSpec as P

MESH = pl.DeviceIdType.MESH
wall_ratio = (1.0 / 9.0) ** (1.0 / 7.0)
steps = [(a, b, c) for a in (-1, 0, 1) for b in (-1, 0, 1) for c in (-1, 0, 1)]
index_of = {e: i for i, e in enumerate(steps)}
weight = [float(np.prod([2.0 / 3.0 if v == 0 else 1.0 / 6.0 for v in e])) for e in steps]
F32 = jnp.float32
I32 = jnp.int32


def along(values, axis, combine):
    stride = (9, 3, 1)[axis]
    out = list(values)
    for i in range(27):
        if i // stride % 3 == 0:
            out[i], out[i + stride], out[i + 2 * stride] = combine(
                values[i], values[i + stride], values[i + 2 * stride]
            )
    return out


def to_moments(lo, mid, hi):
    both = hi + lo
    return both + mid, hi - lo, both


def from_moments(zero, one, two):
    return two - one, zero - two, two + one


def equilibrium_moments(rho, vel):
    sq = [v * v for v in vel]
    third = 1.0 / 3.0
    out = []
    for powers in [(a, b, c) for a in range(3) for b in range(3) for c in range(3)]:
        odd = [k for k in range(3) if powers[k] == 1]
        even = [k for k in range(3) if powers[k] == 2]
        scale = third ** len(even)
        if len(odd) == 3:
            out.append(None)
        elif len(odd) == 2:
            out.append(rho * (vel[odd[0]] * vel[odd[1]] * scale))
        elif len(odd) == 1:
            out.append(rho * (vel[odd[0]] * scale))
        elif not even:
            out.append(rho)
        else:
            total = sq[even[0]]
            for k in even[1:]:
                total = total + sq[k]
            out.append(rho * (scale + 3.0 * scale * total))
    return out


def shifted(value, b, c):
    if c:
        value = pltpu.roll(value, c % 128, 1)
    if b:
        value = pltpu.roll(value, b % 8, 0)
    return value


def lane_gather(table, index):
    return jnp.take_along_axis(table, index, axis=1, mode="promise_in_bounds")


def row_of(ref, lead, row):
    return jnp.broadcast_to(ref[lead + (slice(row, row + 1), slice(None))], (8, 128))


def line(ref, row):
    return jnp.broadcast_to(ref[row], (8, 128))


def total_of(u, e):
    total = None
    for n in range(3):
        if e[n]:
            term = u[n] if e[n] > 0 else -u[n]
            total = term if total is None else total + term
    return total


def body(
    n_gx,
    n_gy,
    pop_h,
    relax_h,
    solid_h,
    cell_h,
    normal_h,
    count_s,
    ref_h,
    corner_h,
    cweight_h,
    out,
    relax_s,
    pop,
    solid,
    cell,
    normal,
    sref,
    corner,
    cweight,
    part,
    fields,
    blocked,
    sample,
    sample_in,
    solid_x,
    solid_y,
    solid_d,
    part_in,
    fields_in,
    rows,
    rows_in,
    rows_d,
    rolled,
    posts,
    edges,
    in_sem,
    tally,
    s_send,
    s_recv,
    h_send,
    h_recv,
    ready,
    whole,
):
    p = lax.axis_index("gx")
    q = lax.axis_index("gy")
    px = [lax.rem(p + n_gx + a, n_gx) for a in (-1, 0, 1)]
    qy = [lax.rem(q + n_gy + b, n_gy) for b in (-1, 0, 1)]
    around = [lax.rem(q + k, n_gy) for k in range(n_gy)]

    loads = [
        pltpu.make_async_copy(src, dst, in_sem.at[k])
        for k, (src, dst) in enumerate(
            [
                (pop_h, pop),
                (corner_h, corner),
                (cweight_h, cweight),
                (relax_h, relax_s),
                (cell_h, cell),
                (normal_h, normal),
                (ref_h, sref),
                (solid_h, solid),
            ]
        )
    ]
    for copy in loads:
        copy.start()

    barrier = pltpu.get_barrier_semaphore()
    by_distance = sorted(range(n_gy), key=lambda k: -min(k, n_gy - k))
    targets = [(a, k) for a in (1, 0, -1) for k in by_distance if a or k]
    for k in by_distance:
        pl.semaphore_signal(
            barrier, inc=1, device_id=(px[0], around[k]), device_id_type=MESH
        )
    row_id = lax.broadcasted_iota(I32, (8, 128), 0)

    pl.semaphore_wait(barrier, n_gy)
    for k in by_distance:
        pl.semaphore_signal(
            ready, inc=1, device_id=(px[2], around[k]), device_id_type=MESH
        )

    vel = []
    for copy in loads[:3]:
        copy.wait()
    for x in range(2):
        f = [pop[i, x] * weight[i] for i in range(27)]
        for axis in (2, 1, 0):
            f = along(f, axis, to_moments)
        rho = f[0]
        inv = 1.0 / rho
        u = [f[9] * inv, f[3] * inv, f[1] * inv]
        vel.append(u)
        fields[0, x] = rho
        for k in range(3):
            fields[k + 1, x] = u[k]
        for m in range(27):
            part[m, x] = f[m]

    for j in range(4):
        total = [jnp.zeros((8, 128), F32) for _ in range(3)]
        lanes = slice(128 * j, 128 * (j + 1))
        for k in range(8):
            where = jnp.broadcast_to(corner[0, 0, k : k + 1, lanes], (8, 128))
            share = jnp.broadcast_to(cweight[0, 0, k : k + 1, lanes], (8, 128))
            lane = where & 127
            mine = jnp.where((where >> 7) & 7 == row_id, share, 0.0)
            upper = where >= 1024
            for n in range(3):
                got = jnp.where(upper, lane_gather(vel[1][n], lane), lane_gather(vel[0][n], lane))
                total[n] = total[n] + mine * got
        for n in range(3):
            summed = jnp.sum(total[n], axis=0, keepdims=True)
            sample[3 * j + n] = summed
            if j == 0:
                sample[12 + n] = summed

    par = lax.rem(q, 2)

    def window(d):
        return 3 * lax.div(lax.rem(d + n_gy - 1, n_gy), 2)

    mine = window(q)
    for r in range(6):
        sample_in[(n_gy + q) * 6 + r] = sample[mine + r]

    def send(src, dst, send_sem, recv_sem, peer):
        pltpu.make_async_remote_copy(
            src_ref=src, dst_ref=dst, send_sem=send_sem, recv_sem=recv_sem,
            device_id=peer, device_id_type=MESH,
        ).start()

    def send_samples(a):
        for b, k in targets:
            if b == a:
                send(
                    sample.at[pl.ds(window(around[k]), 6)],
                    sample_in.at[pl.ds(((1 - a) * n_gy + q) * 6, 6)],
                    s_send,
                    s_recv.at[1 - a],
                    (px[a + 1], around[k]),
                )

    def send_side(n):
        a = 1 - 2 * n
        x = 1 - n
        to = px[a + 1]
        halo = []
        for m, b in enumerate((1, -1)):
            halo.append(
                (rows.at[pl.ds(42 * m + 24 + 9 * n, 9)], rows_d.at[pl.ds((2 * n + m) * 9, 9)], (to, qy[b + 1]))
            )
        halo.append((fields.at[:, x], fields_in.at[n], (to, q)))
        halo.append((part.at[pl.ds(18 - 18 * n, 9), x], part_in.at[n], (to, q)))
        halo.append((solid.at[x], solid_x.at[n], (to, q)))
        for m, b in enumerate((1, -1)):
            halo.append((solid.at[x], solid_d.at[n, m], (to, qy[b + 1])))
        for src, dst, peer in halo:
            send(src, dst, h_send, h_recv.at[n], peer)

    def send_row():
        for m, b in enumerate((1, -1)):
            to = (p, qy[b + 1])
            send(rows.at[pl.ds(42 * m, 24)], rows_in.at[pl.ds(24 * m, 24)], h_send, h_recv.at[2], to)
            send(solid, solid_y.at[m], h_send, h_recv.at[2], to)

    def arrived(sem, lines):
        span = tally.at[pl.ds(0, lines)]
        pltpu.make_async_copy(span, span, sem).wait()

    side_lines = 2 * 9 + 48 + 72 + 24
    row_lines = 2 * (24 + 16)

    send_samples(1)

    for copy in loads[4:]:
        copy.wait()
    cells = cell[0]
    live = lax.broadcasted_iota(I32, (1, 512), 1) < count_s[0, 0]
    refs = sref[0]
    first = jnp.where(live, (refs & 63) + 1, 0)
    second = jnp.where(live, (refs >> 6) * 8 + normal[0], 0)
    rows16 = lax.broadcasted_iota(I32, (16, 512), 0) == (cells >> 7)
    left = jnp.concatenate(
        [jnp.where(rows16, first, 0), jnp.where(rows16, second, 0)], axis=0
    ).astype(F32).astype(jnp.bfloat16)
    right = jnp.where(
        lax.broadcasted_iota(I32, (128, 512), 0) == (cells & 127), 1.0, 0.0
    ).astype(jnp.bfloat16)
    code = lax.dot_general(
        left, right, (((1,), (1,)), ((), ())), preferred_element_type=F32
    ).astype(I32)
    slot = code[0:16]
    owner = code[16:32]
    use = jnp.where(slot > 0, (owner >> 3) * 64 + slot, 0).astype(F32)
    axes = ((owner & 7) >> 1).astype(F32)
    for x in range(2):
        fields[4, x] = use[8 * x : 8 * x + 8]
        fields[5, x] = axes[8 * x : 8 * x + 8]

    loads[3].wait()
    for x in range(2):
        f = [part[m, x] for m in range(27)]
        balance = equilibrium_moments(fields[0, x], [fields[1 + k, x] for k in range(3)])
        for m in range(27):
            off = f[m] if balance[m] is None else f[m] - balance[m]
            f[m] = off * (1.0 - relax_s[m])
        for axis in (2, 1, 0):
            f = along(f, axis, from_moments)
        for i, e in enumerate(steps):
            part[i, x] = f[i] * float(np.prod([1.5 if v == 0 else 3.0 for v in e]))

    for m, b in enumerate((1, -1)):
        near = slice(7, 8) if b == 1 else slice(0, 1)
        base = 42 * m
        for c in (-1, 0, 1):
            for s, (a, x) in enumerate(((0, 0), (0, 1), (1, 0), (-1, 1))):
                rows[base + 4 * (c + 1) + s] = part[index_of[a, b, c], x, near]
            for n, (a, x) in enumerate(((1, 1), (-1, 0))):
                rows[base + 24 + 9 * n + c + 1] = part[index_of[a, b, c], x, near]
        for k in range(6):
            for x in range(2):
                value = fields[k, x, near]
                rows[base + 12 + 6 * x + k] = value
                rows[base + 27 + 9 * (1 - x) + k] = value

    send_side(0)
    def greet():
        pl.semaphore_wait(ready, n_gy)
        pl.semaphore_signal(whole, inc=1, device_id=(px[0], q), device_id_type=MESH)

    def send_back():
        send_samples(-1)
        send_side(1)

    pl.when(p != 0)(greet)
    pl.semaphore_wait(whole, 1)
    send_samples(0)
    send_row()
    pl.when(p != 0)(send_back)

    chunk = [0, 1 - par, 1]
    half = [1 - par, par, 1 - par]

    def table(g, t, k, n):
        return line(sample_in, (g * n_gy + around[k]) * 6 + 3 * chunk[t] + n)

    def wall_velocity(use, axis, u, tables, lanes):
        use = use.astype(I32)
        spot = use - 1
        who = spot >> 6
        lane = (spot & 63) + lanes
        picked = [jnp.zeros((8, 128), F32) for _ in range(3)]
        for k in reversed(by_distance):
            here = who == around[k]
            for n in range(3):
                picked[n] = jnp.where(here, lane_gather(tables(k, n), lane), picked[n])
        return [
            jnp.where(use > 0, jnp.where(axis == float(n), 0.0, wall_ratio * picked[n]), u[n])
            for n in range(3)
        ]

    def base_of(rho, u):
        return rho - 1.5 * rho * (u[0] * u[0] + u[1] * u[1] + u[2] * u[2])

    arrived(s_recv.at[1], (n_gy - 1) * 6)
    for x in range(2):
        rho = fields[0, x]
        u = wall_velocity(
            fields[4, x], fields[5, x], [fields[1 + n, x] for n in range(3)],
            lambda k, n: table(1, 1, k, n), half[1] * 64,
        )
        base = base_of(rho, u)
        for i in range(13, 27):
            along_e = total_of(u, steps[i])
            if along_e is None:
                posts[i, x] = part[i, x] + base
                continue
            linear = 3.0 * rho * along_e
            even = base + 1.5 * along_e * linear
            posts[i, x] = part[i, x] + (even + linear)
            posts[26 - i, x] = part[26 - i, x] + (even - linear)
    for i, (a, b, c) in enumerate(steps):
        for x in range(2):
            if 0 <= x + a <= 1:
                rolled[i, x] = shifted(posts[i, x], b, c)

    def side(n):
        a = 1 - 2 * n
        rho = fields_in[n, 0]
        u = wall_velocity(
            fields_in[n, 4], fields_in[n, 5], [fields_in[n, 1 + k] for k in range(3)],
            lambda k, m: table(2 * n, 1, k, m), half[1] * 64,
        )
        base = base_of(rho, u)
        for s, (b, c) in enumerate((b, c) for b in (-1, 0, 1) for c in (-1, 0, 1)):
            along_e = total_of(u, (a, b, c))
            linear = 3.0 * rho * along_e
            value = part_in[n, s] + (base + linear + 1.5 * along_e * linear)
            rolled[index_of[a, b, c], 1 - n] = shifted(value, b, c)

    def block_plane(xx, plane):
        for b in (-1, 0, 1):
            moved = plane
            if b:
                m = 0 if b == 1 else 1
                near = 7 if b == 1 else 0
                if xx in (1, 2):
                    edge = row_of(solid_y, (m, xx - 1), near)
                else:
                    edge = row_of(solid_d, (0 if xx == 0 else 1, m), near)
                moved = pltpu.roll(plane, b % 8, 0)
                moved = jnp.where(row_id == (0 if b == 1 else 7), edge, moved)
            for c in (-1, 0, 1):
                blocked[xx, 3 * (b + 1) + c + 1] = shifted(moved, 0, c)

    at = [row_id == s for s in range(8)]
    lower = row_id < 4
    across = row_id & 3

    def gather_rows(entries):
        value = None
        for s, piece in entries:
            value = piece if value is None else jnp.where(at[s], piece, value)
        return value

    def field_row(k, near):
        entries = []
        for m in range(2):
            if near:
                entries.append((4 * m + 1, line(rows_in, m * 24 + 12 + k)))
                entries.append((4 * m + 2, line(rows_in, m * 24 + 18 + k)))
                entries.append((4 * m + 3, line(rows_d, (2 + m) * 9 + 3 + k)))
            else:
                entries.append((4 * m, line(rows_d, m * 9 + 3 + k)))
        return gather_rows(entries)

    def part_row(a, c, near):
        entries = []
        for m in range(2):
            base = m * 24 + 4 * (c + 1)
            if not near:
                entries.append((4 * m, line(rows_d, m * 9 + c + 1)))
            elif a == 0:
                entries.append((4 * m + 1, line(rows_in, base)))
                entries.append((4 * m + 2, line(rows_in, base + 1)))
            elif a == 1:
                entries.append((4 * m + 1, line(rows_in, base + 2)))
            else:
                entries.append((4 * m + 2, line(rows_in, base + 3)))
                entries.append((4 * m + 3, line(rows_d, (2 + m) * 9 + c + 1)))
        return gather_rows(entries)

    def table_near(k, n):
        value = jnp.where(lower, table(1, 0, k, n), table(1, 2, k, n))
        other = jnp.where(lower, table(2, 0, k, n), table(2, 2, k, n))
        return jnp.where(across == 3, other, value)

    def table_far(k, n):
        return jnp.where(lower, table(0, 0, k, n), table(0, 2, k, n))

    def edge_rows(found, parts, tables, where):
        rho = found[0]
        u = wall_velocity(found[4], found[5], found[1:4], tables, (1 - par) * 64)
        base = base_of(rho, u)
        u = [u[0], jnp.where(lower, u[1], -u[1]), u[2]]
        for (a, c), piece in parts.items():
            along_e = total_of(u, (a, 1, c))
            linear = 3.0 * rho * along_e
            value = piece + (base + linear + 1.5 * along_e * linear)
            edges[where + 3 * (a + 1) + c + 1] = shifted(value, 0, c)

    def finish(far):
        for i, (a, b, c) in enumerate(steps):
            for x in range(2):
                xx = x - a
                if (xx == -1) != far:
                    continue
                value = rolled[i, xx if 0 <= xx <= 1 else 1 if a == 1 else 0]
                if b:
                    m = 0 if b == 1 else 1
                    s = (9 if far else 0) + 3 * (a + 1) + c + 1
                    edge = row_of(edges, (s,), 4 * m + xx + 1)
                    value = jnp.where(row_id == (0 if b == 1 else 7), edge, value)
                wall = blocked[xx + 1, 3 * (b + 1) + c + 1]
                out[i, x] = jnp.where(wall != 0, posts[26 - i, x], value)

    arrived(h_recv.at[2], row_lines)
    arrived(h_recv.at[1], side_lines)
    for xx, plane in ((1, solid[0]), (2, solid[1]), (3, solid_x[1])):
        block_plane(xx, plane)
    found = [field_row(k, True) for k in range(6)]
    parts = {(a, c): part_row(a, c, True) for a in (-1, 0, 1) for c in (-1, 0, 1)}
    arrived(s_recv.at[2], n_gy * 6)
    side(1)
    edge_rows(found, parts, table_near, 0)
    finish(False)

    @pl.when(p == 0)
    def _():
        greet()
        send_back()

    arrived(h_recv.at[0], side_lines)
    block_plane(0, solid_x[0])
    found = [field_row(k, False) for k in range(6)]
    parts = {(1, c): part_row(1, c, False) for c in (-1, 0, 1)}
    arrived(s_recv.at[0], n_gy * 6)
    side(0)
    edge_rows(found, parts, table_far, 9)
    finish(True)

    arrived(s_send, len(targets) * 6)
    arrived(h_send, 2 * side_lines + row_lines)


def local(*args):
    n_gx, n_gy = lax.axis_size("gx"), lax.axis_size("gy")
    hbm = pl.BlockSpec(memory_space=pl.ANY)
    smem = pl.BlockSpec(memory_space=pltpu.SMEM)
    vmem = pltpu.VMEM
    dma = pltpu.SemaphoreType.DMA
    args = [
        a if k == 5 else pltpu.with_memory_space_constraint(a, pltpu.HBM)
        for k, a in enumerate(args)
    ]
    return pl.pallas_call(
        lambda *refs: body(n_gx, n_gy, *refs),
        name="lattice_step",
        out_shape=vmem((27, 2, 8, 128), F32),
        in_specs=[hbm, hbm, hbm, hbm, hbm, smem, hbm, hbm, hbm],
        out_specs=pl.BlockSpec(memory_space=pltpu.VMEM),
        scratch_shapes=[
            pltpu.SMEM((27,), F32),
            vmem((27, 2, 8, 128), F32),
            vmem((2, 8, 128), I32),
            vmem((1, 1, 512), I32),
            vmem((1, 1, 512), I32),
            vmem((1, 1, 512), I32),
            vmem((1, 1, 8, 512), I32),
            vmem((1, 1, 8, 512), F32),
            vmem((27, 2, 8, 128), F32),
            vmem((6, 2, 8, 128), F32),
            vmem((4, 9, 8, 128), I32),
            vmem((15, 1, 128), F32),
            vmem((3 * n_gy * 6, 1, 128), F32),
            vmem((2, 8, 128), I32),
            vmem((2, 2, 8, 128), I32),
            vmem((2, 2, 8, 128), I32),
            vmem((2, 9, 8, 128), F32),
            vmem((2, 6, 8, 128), F32),
            vmem((84, 1, 128), F32),
            vmem((48, 1, 128), F32),
            vmem((36, 1, 128), F32),
            vmem((27, 2, 8, 128), F32),
            vmem((27, 2, 8, 128), F32),
            vmem((18, 8, 128), F32),
            dma((8,)),
            vmem((404, 1, 128), F32),
            dma(()),
            dma((3,)),
            dma(()),
            dma((3,)),
            pltpu.SemaphoreType.REGULAR,
            pltpu.SemaphoreType.REGULAR,
        ],
        compiler_params=pltpu.CompilerParams(
            collective_id=0, has_side_effects=True, vmem_limit_bytes=16 << 20
        ),
    )(*args)


def solution(mesh):
    return jax.shard_map(
        local,
        mesh=mesh,
        in_specs=(
            P(None, "gx", "gy", None),
            P(),
            P("gx", "gy", None),
            P("gx", "gy", None),
            P("gx", "gy", None),
            P("gx", "gy"),
            P("gx", "gy", None),
            P("gx", "gy", None, None),
            P("gx", "gy", None, None),
        ),
        out_specs=P(None, "gx", "gy", None),
        check_vma=False,
    )
```

```python
import jax
import jax.numpy as jnp
import numpy as np
from jax import lax
from jax.experimental import pallas as pl
from jax.experimental.pallas import tpu as pltpu
from jax.sharding import PartitionSpec as P

MESH = pl.DeviceIdType.MESH
wall_ratio = (1.0 / 9.0) ** (1.0 / 7.0)
steps = [(a, b, c) for a in (-1, 0, 1) for b in (-1, 0, 1) for c in (-1, 0, 1)]
index_of = {e: i for i, e in enumerate(steps)}
weight = [float(np.prod([2.0 / 3.0 if v == 0 else 1.0 / 6.0 for v in e])) for e in steps]
F32 = jnp.float32
I32 = jnp.int32


def along(values, axis, combine):
    stride = (9, 3, 1)[axis]
    out = list(values)
    for i in range(27):
        if i // stride % 3 == 0:
            out[i], out[i + stride], out[i + 2 * stride] = combine(
                values[i], values[i + stride], values[i + 2 * stride]
            )
    return out


def to_moments(lo, mid, hi):
    both = hi + lo
    return both + mid, hi - lo, both


def from_moments(zero, one, two):
    return two - one, zero - two, two + one


def equilibrium_moments(rho, vel):
    sq = [v * v for v in vel]
    third = 1.0 / 3.0
    out = []
    for powers in [(a, b, c) for a in range(3) for b in range(3) for c in range(3)]:
        odd = [k for k in range(3) if powers[k] == 1]
        even = [k for k in range(3) if powers[k] == 2]
        scale = third ** len(even)
        if len(odd) == 3:
            out.append(None)
        elif len(odd) == 2:
            out.append(rho * (vel[odd[0]] * vel[odd[1]] * scale))
        elif len(odd) == 1:
            out.append(rho * (vel[odd[0]] * scale))
        elif not even:
            out.append(rho)
        else:
            total = sq[even[0]]
            for k in even[1:]:
                total = total + sq[k]
            out.append(rho * (scale + 3.0 * scale * total))
    return out


def shifted(value, b, c):
    if c:
        value = pltpu.roll(value, c % 128, 1)
    if b:
        value = pltpu.roll(value, b % 8, 0)
    return value


def lane_gather(table, index):
    return jnp.take_along_axis(table, index, axis=1, mode="promise_in_bounds")


def row_of(ref, lead, row):
    return jnp.broadcast_to(ref[lead + (slice(row, row + 1), slice(None))], (8, 128))


def line(ref, row):
    return jnp.broadcast_to(ref[row], (8, 128))


def total_of(u, e):
    total = None
    for n in range(3):
        if e[n]:
            term = u[n] if e[n] > 0 else -u[n]
            total = term if total is None else total + term
    return total


def body(
    n_gx,
    n_gy,
    pop_h,
    relax_h,
    solid_h,
    cell_h,
    normal_h,
    count_s,
    ref_h,
    corner_h,
    cweight_h,
    out,
    relax_s,
    pop,
    solid,
    cell,
    normal,
    sref,
    corner,
    cweight,
    part,
    fields,
    blocked,
    sample,
    sample_in,
    solid_x,
    solid_y,
    solid_d,
    part_in,
    fields_in,
    rows,
    rows_in,
    rows_d,
    rolled,
    posts,
    edges,
    in_sem,
    tally,
    s_send,
    s_recv,
    h_send,
    h_recv,
    ready,
    whole,
):
    p = lax.axis_index("gx")
    q = lax.axis_index("gy")
    px = [lax.rem(p + n_gx + a, n_gx) for a in (-1, 0, 1)]
    qy = [lax.rem(q + n_gy + b, n_gy) for b in (-1, 0, 1)]
    around = [lax.rem(q + k, n_gy) for k in range(n_gy)]

    loads = [
        pltpu.make_async_copy(src, dst, in_sem.at[k])
        for k, (src, dst) in enumerate(
            [
                (pop_h, pop),
                (corner_h, corner),
                (cweight_h, cweight),
                (relax_h, relax_s),
                (cell_h, cell),
                (normal_h, normal),
                (ref_h, sref),
                (solid_h, solid),
            ]
        )
    ]
    for copy in loads:
        copy.start()

    barrier = pltpu.get_barrier_semaphore()
    by_distance = sorted(range(n_gy), key=lambda k: -min(k, n_gy - k))
    targets = [(a, k) for a in (1, 0, -1) for k in by_distance if a or k]
    for k in by_distance:
        pl.semaphore_signal(
            barrier, inc=1, device_id=(px[0], around[k]), device_id_type=MESH
        )
    row_id = lax.broadcasted_iota(I32, (8, 128), 0)

    pl.semaphore_wait(barrier, n_gy)
    for k in by_distance:
        pl.semaphore_signal(
            ready, inc=1, device_id=(px[2], around[k]), device_id_type=MESH
        )

    vel = []
    for copy in loads[:3]:
        copy.wait()
    for x in range(2):
        f = [pop[i, x] * weight[i] for i in range(27)]
        for axis in (2, 1, 0):
            f = along(f, axis, to_moments)
        rho = f[0]
        inv = 1.0 / rho
        u = [f[9] * inv, f[3] * inv, f[1] * inv]
        vel.append(u)
        fields[0, x] = rho
        for k in range(3):
            fields[k + 1, x] = u[k]

    for j in range(4):
        total = [jnp.zeros((8, 128), F32) for _ in range(3)]
        lanes = slice(128 * j, 128 * (j + 1))
        for k in range(8):
            where = jnp.broadcast_to(corner[0, 0, k : k + 1, lanes], (8, 128))
            share = jnp.broadcast_to(cweight[0, 0, k : k + 1, lanes], (8, 128))
            lane = where & 127
            mine = jnp.where((where >> 7) & 7 == row_id, share, 0.0)
            upper = where >= 1024
            for n in range(3):
                got = jnp.where(upper, lane_gather(vel[1][n], lane), lane_gather(vel[0][n], lane))
                total[n] = total[n] + mine * got
        for n in range(3):
            summed = jnp.sum(total[n], axis=0, keepdims=True)
            sample[3 * j + n] = summed
            if j == 0:
                sample[12 + n] = summed

    par = lax.rem(q, 2)

    def window(d):
        return 3 * lax.div(lax.rem(d + n_gy - 1, n_gy), 2)

    mine = window(q)
    for r in range(6):
        sample_in[(n_gy + q) * 6 + r] = sample[mine + r]

    def send(src, dst, send_sem, recv_sem, peer):
        pltpu.make_async_remote_copy(
            src_ref=src, dst_ref=dst, send_sem=send_sem, recv_sem=recv_sem,
            device_id=peer, device_id_type=MESH,
        ).start()

    def send_samples(a):
        for b, k in targets:
            if b == a:
                send(
                    sample.at[pl.ds(window(around[k]), 6)],
                    sample_in.at[pl.ds(((1 - a) * n_gy + q) * 6, 6)],
                    s_send,
                    s_recv.at[1 - a],
                    (px[a + 1], around[k]),
                )

    def send_side(n):
        a = 1 - 2 * n
        x = 1 - n
        to = px[a + 1]
        halo = []
        for m, b in enumerate((1, -1)):
            halo.append(
                (rows.at[pl.ds(42 * m + 24 + 9 * n, 9)], rows_d.at[pl.ds((2 * n + m) * 9, 9)], (to, qy[b + 1]))
            )
        halo.append((fields.at[:, x], fields_in.at[n], (to, q)))
        halo.append((part.at[pl.ds(18 - 18 * n, 9), x], part_in.at[n], (to, q)))
        halo.append((solid.at[x], solid_x.at[n], (to, q)))
        for m, b in enumerate((1, -1)):
            halo.append((solid.at[x], solid_d.at[n, m], (to, qy[b + 1])))
        for src, dst, peer in halo:
            send(src, dst, h_send, h_recv.at[n], peer)

    def send_row():
        for m, b in enumerate((1, -1)):
            to = (p, qy[b + 1])
            send(rows.at[pl.ds(42 * m, 24)], rows_in.at[pl.ds(24 * m, 24)], h_send, h_recv.at[2], to)
            send(solid, solid_y.at[m], h_send, h_recv.at[2], to)

    def arrived(sem, lines):
        span = tally.at[pl.ds(0, lines)]
        pltpu.make_async_copy(span, span, sem).wait()

    side_lines = 2 * 9 + 48 + 72 + 24
    row_lines = 2 * (24 + 16)

    send_samples(1)

    for copy in loads[4:]:
        copy.wait()
    cells = cell[0]
    live = lax.broadcasted_iota(I32, (1, 512), 1) < count_s[0, 0]
    refs = sref[0]
    first = jnp.where(live, (refs & 63) + 1, 0)
    second = jnp.where(live, (refs >> 6) * 8 + normal[0], 0)
    rows16 = lax.broadcasted_iota(I32, (16, 512), 0) == (cells >> 7)
    left = jnp.concatenate(
        [jnp.where(rows16, first, 0), jnp.where(rows16, second, 0)], axis=0
    ).astype(F32).astype(jnp.bfloat16)
    right = jnp.where(
        lax.broadcasted_iota(I32, (128, 512), 0) == (cells & 127), 1.0, 0.0
    ).astype(jnp.bfloat16)
    code = lax.dot_general(
        left, right, (((1,), (1,)), ((), ())), preferred_element_type=F32
    ).astype(I32)
    slot = code[0:16]
    owner = code[16:32]
    use = jnp.where(slot > 0, (owner >> 3) * 64 + slot, 0).astype(F32)
    axes = ((owner & 7) >> 1).astype(F32)
    for x in range(2):
        fields[4, x] = use[8 * x : 8 * x + 8]
        fields[5, x] = axes[8 * x : 8 * x + 8]

    loads[3].wait()
    for x in range(2):
        f = [pop[i, x] * weight[i] for i in range(27)]
        for axis in (2, 1, 0):
            f = along(f, axis, to_moments)
        balance = equilibrium_moments(fields[0, x], [fields[1 + k, x] for k in range(3)])
        for m in range(27):
            off = f[m] if balance[m] is None else f[m] - balance[m]
            f[m] = off * (1.0 - relax_s[m])
        for axis in (2, 1, 0):
            f = along(f, axis, from_moments)
        for i, e in enumerate(steps):
            part[i, x] = f[i] * float(np.prod([1.5 if v == 0 else 3.0 for v in e]))

    for m, b in enumerate((1, -1)):
        near = slice(7, 8) if b == 1 else slice(0, 1)
        base = 42 * m
        for c in (-1, 0, 1):
            for s, (a, x) in enumerate(((0, 0), (0, 1), (1, 0), (-1, 1))):
                rows[base + 4 * (c + 1) + s] = part[index_of[a, b, c], x, near]
            for n, (a, x) in enumerate(((1, 1), (-1, 0))):
                rows[base + 24 + 9 * n + c + 1] = part[index_of[a, b, c], x, near]
        for k in range(6):
            for x in range(2):
                value = fields[k, x, near]
                rows[base + 12 + 6 * x + k] = value
                rows[base + 27 + 9 * (1 - x) + k] = value

    send_side(0)
    def greet():
        pl.semaphore_wait(ready, n_gy)
        pl.semaphore_signal(whole, inc=1, device_id=(px[0], q), device_id_type=MESH)

    def send_back():
        send_samples(-1)
        send_side(1)

    pl.when(p != 0)(greet)
    pl.semaphore_wait(whole, 1)
    send_samples(0)
    send_row()
    pl.when(p != 0)(send_back)

    chunk = [0, 1 - par, 1]
    half = [1 - par, par, 1 - par]

    def table(g, t, k, n):
        return line(sample_in, (g * n_gy + around[k]) * 6 + 3 * chunk[t] + n)

    def wall_velocity(use, axis, u, tables, lanes):
        use = use.astype(I32)
        spot = use - 1
        who = spot >> 6
        lane = (spot & 63) + lanes
        picked = [jnp.zeros((8, 128), F32) for _ in range(3)]
        for k in reversed(by_distance):
            here = who == around[k]
            for n in range(3):
                picked[n] = jnp.where(here, lane_gather(tables(k, n), lane), picked[n])
        return [
            jnp.where(use > 0, jnp.where(axis == float(n), 0.0, wall_ratio * picked[n]), u[n])
            for n in range(3)
        ]

    def base_of(rho, u):
        return rho - 1.5 * rho * (u[0] * u[0] + u[1] * u[1] + u[2] * u[2])

    arrived(s_recv.at[1], (n_gy - 1) * 6)
    for x in range(2):
        rho = fields[0, x]
        u = wall_velocity(
            fields[4, x], fields[5, x], [fields[1 + n, x] for n in range(3)],
            lambda k, n: table(1, 1, k, n), half[1] * 64,
        )
        base = base_of(rho, u)
        for i in range(13, 27):
            along_e = total_of(u, steps[i])
            if along_e is None:
                posts[i, x] = part[i, x] + base
                continue
            linear = 3.0 * rho * along_e
            even = base + 1.5 * along_e * linear
            posts[i, x] = part[i, x] + (even + linear)
            posts[26 - i, x] = part[26 - i, x] + (even - linear)
    for i, (a, b, c) in enumerate(steps):
        for x in range(2):
            if 0 <= x + a <= 1:
                rolled[i, x] = shifted(posts[i, x], b, c)

    def side(n):
        a = 1 - 2 * n
        rho = fields_in[n, 0]
        u = wall_velocity(
            fields_in[n, 4], fields_in[n, 5], [fields_in[n, 1 + k] for k in range(3)],
            lambda k, m: table(2 * n, 1, k, m), half[1] * 64,
        )
        base = base_of(rho, u)
        for s, (b, c) in enumerate((b, c) for b in (-1, 0, 1) for c in (-1, 0, 1)):
            along_e = total_of(u, (a, b, c))
            linear = 3.0 * rho * along_e
            value = part_in[n, s] + (base + linear + 1.5 * along_e * linear)
            rolled[index_of[a, b, c], 1 - n] = shifted(value, b, c)

    def block_plane(xx, plane):
        for b in (-1, 0, 1):
            moved = plane
            if b:
                m = 0 if b == 1 else 1
                near = 7 if b == 1 else 0
                if xx in (1, 2):
                    edge = row_of(solid_y, (m, xx - 1), near)
                else:
                    edge = row_of(solid_d, (0 if xx == 0 else 1, m), near)
                moved = pltpu.roll(plane, b % 8, 0)
                moved = jnp.where(row_id == (0 if b == 1 else 7), edge, moved)
            for c in (-1, 0, 1):
                blocked[xx, 3 * (b + 1) + c + 1] = shifted(moved, 0, c)

    at = [row_id == s for s in range(8)]
    lower = row_id < 4
    across = row_id & 3

    def gather_rows(entries):
        value = None
        for s, piece in entries:
            value = piece if value is None else jnp.where(at[s], piece, value)
        return value

    def field_row(k, near):
        entries = []
        for m in range(2):
            if near:
                entries.append((4 * m + 1, line(rows_in, m * 24 + 12 + k)))
                entries.append((4 * m + 2, line(rows_in, m * 24 + 18 + k)))
                entries.append((4 * m + 3, line(rows_d, (2 + m) * 9 + 3 + k)))
            else:
                entries.append((4 * m, line(rows_d, m * 9 + 3 + k)))
        return gather_rows(entries)

    def part_row(a, c, near):
        entries = []
        for m in range(2):
            base = m * 24 + 4 * (c + 1)
            if not near:
                entries.append((4 * m, line(rows_d, m * 9 + c + 1)))
            elif a == 0:
                entries.append((4 * m + 1, line(rows_in, base)))
                entries.append((4 * m + 2, line(rows_in, base + 1)))
            elif a == 1:
                entries.append((4 * m + 1, line(rows_in, base + 2)))
            else:
                entries.append((4 * m + 2, line(rows_in, base + 3)))
                entries.append((4 * m + 3, line(rows_d, (2 + m) * 9 + c + 1)))
        return gather_rows(entries)

    def table_near(k, n):
        value = jnp.where(lower, table(1, 0, k, n), table(1, 2, k, n))
        other = jnp.where(lower, table(2, 0, k, n), table(2, 2, k, n))
        return jnp.where(across == 3, other, value)

    def table_far(k, n):
        return jnp.where(lower, table(0, 0, k, n), table(0, 2, k, n))

    def edge_rows(found, parts, tables, where):
        rho = found[0]
        u = wall_velocity(found[4], found[5], found[1:4], tables, (1 - par) * 64)
        base = base_of(rho, u)
        u = [u[0], jnp.where(lower, u[1], -u[1]), u[2]]
        for (a, c), piece in parts.items():
            along_e = total_of(u, (a, 1, c))
            linear = 3.0 * rho * along_e
            value = piece + (base + linear + 1.5 * along_e * linear)
            edges[where + 3 * (a + 1) + c + 1] = shifted(value, 0, c)

    def finish(far):
        for i, (a, b, c) in enumerate(steps):
            for x in range(2):
                xx = x - a
                if (xx == -1) != far:
                    continue
                value = rolled[i, xx if 0 <= xx <= 1 else 1 if a == 1 else 0]
                if b:
                    m = 0 if b == 1 else 1
                    s = (9 if far else 0) + 3 * (a + 1) + c + 1
                    edge = row_of(edges, (s,), 4 * m + xx + 1)
                    value = jnp.where(row_id == (0 if b == 1 else 7), edge, value)
                wall = blocked[xx + 1, 3 * (b + 1) + c + 1]
                out[i, x] = jnp.where(wall != 0, posts[26 - i, x], value)

    arrived(h_recv.at[2], row_lines)
    arrived(h_recv.at[1], side_lines)
    for xx, plane in ((1, solid[0]), (2, solid[1]), (3, solid_x[1])):
        block_plane(xx, plane)
    found = [field_row(k, True) for k in range(6)]
    parts = {(a, c): part_row(a, c, True) for a in (-1, 0, 1) for c in (-1, 0, 1)}
    arrived(s_recv.at[2], n_gy * 6)
    side(1)
    edge_rows(found, parts, table_near, 0)
    finish(False)

    @pl.when(p == 0)
    def _():
        greet()
        send_back()

    arrived(h_recv.at[0], side_lines)
    block_plane(0, solid_x[0])
    found = [field_row(k, False) for k in range(6)]
    parts = {(1, c): part_row(1, c, False) for c in (-1, 0, 1)}
    arrived(s_recv.at[0], n_gy * 6)
    side(0)
    edge_rows(found, parts, table_far, 9)
    finish(True)

    arrived(s_send, len(targets) * 6)
    arrived(h_send, 2 * side_lines + row_lines)


def local(*args):
    n_gx, n_gy = lax.axis_size("gx"), lax.axis_size("gy")
    hbm = pl.BlockSpec(memory_space=pl.ANY)
    smem = pl.BlockSpec(memory_space=pltpu.SMEM)
    vmem = pltpu.VMEM
    dma = pltpu.SemaphoreType.DMA
    args = [
        a if k == 5 else pltpu.with_memory_space_constraint(a, pltpu.HBM)
        for k, a in enumerate(args)
    ]
    return pl.pallas_call(
        lambda *refs: body(n_gx, n_gy, *refs),
        name="lattice_step",
        out_shape=vmem((27, 2, 8, 128), F32),
        in_specs=[hbm, hbm, hbm, hbm, hbm, smem, hbm, hbm, hbm],
        out_specs=pl.BlockSpec(memory_space=pltpu.VMEM),
        scratch_shapes=[
            pltpu.SMEM((27,), F32),
            vmem((27, 2, 8, 128), F32),
            vmem((2, 8, 128), I32),
            vmem((1, 1, 512), I32),
            vmem((1, 1, 512), I32),
            vmem((1, 1, 512), I32),
            vmem((1, 1, 8, 512), I32),
            vmem((1, 1, 8, 512), F32),
            vmem((27, 2, 8, 128), F32),
            vmem((6, 2, 8, 128), F32),
            vmem((4, 9, 8, 128), I32),
            vmem((15, 1, 128), F32),
            vmem((3 * n_gy * 6, 1, 128), F32),
            vmem((2, 8, 128), I32),
            vmem((2, 2, 8, 128), I32),
            vmem((2, 2, 8, 128), I32),
            vmem((2, 9, 8, 128), F32),
            vmem((2, 6, 8, 128), F32),
            vmem((84, 1, 128), F32),
            vmem((48, 1, 128), F32),
            vmem((36, 1, 128), F32),
            vmem((27, 2, 8, 128), F32),
            vmem((27, 2, 8, 128), F32),
            vmem((18, 8, 128), F32),
            dma((8,)),
            vmem((404, 1, 128), F32),
            dma(()),
            dma((3,)),
            dma(()),
            dma((3,)),
            pltpu.SemaphoreType.REGULAR,
            pltpu.SemaphoreType.REGULAR,
        ],
        compiler_params=pltpu.CompilerParams(
            collective_id=0, has_side_effects=True, vmem_limit_bytes=16 << 20
        ),
    )(*args)


def solution(mesh):
    return jax.shard_map(
        local,
        mesh=mesh,
        in_specs=(
            P(None, "gx", "gy", None),
            P(),
            P("gx", "gy", None),
            P("gx", "gy", None),
            P("gx", "gy", None),
            P("gx", "gy"),
            P("gx", "gy", None),
            P("gx", "gy", None, None),
            P("gx", "gy", None, None),
        ),
        out_specs=P(None, "gx", "gy", None),
        check_vma=False,
    )
```

```python
import jax
import jax.numpy as jnp
import numpy as np
from jax import lax
from jax.experimental import pallas as pl
from jax.experimental.pallas import tpu as pltpu
from jax.sharding import PartitionSpec as P

MESH = pl.DeviceIdType.MESH
wall_ratio = (1.0 / 9.0) ** (1.0 / 7.0)
steps = [(a, b, c) for a in (-1, 0, 1) for b in (-1, 0, 1) for c in (-1, 0, 1)]
index_of = {e: i for i, e in enumerate(steps)}
weight = [float(np.prod([2.0 / 3.0 if v == 0 else 1.0 / 6.0 for v in e])) for e in steps]
F32 = jnp.float32
I32 = jnp.int32


def along(values, axis, combine):
    stride = (9, 3, 1)[axis]
    out = list(values)
    for i in range(27):
        if i // stride % 3 == 0:
            out[i], out[i + stride], out[i + 2 * stride] = combine(
                values[i], values[i + stride], values[i + 2 * stride]
            )
    return out


def to_moments(lo, mid, hi):
    both = hi + lo
    return both + mid, hi - lo, both


def from_moments(zero, one, two):
    return two - one, zero - two, two + one


def equilibrium_moments(rho, vel):
    sq = [v * v for v in vel]
    third = 1.0 / 3.0
    out = []
    for powers in [(a, b, c) for a in range(3) for b in range(3) for c in range(3)]:
        odd = [k for k in range(3) if powers[k] == 1]
        even = [k for k in range(3) if powers[k] == 2]
        scale = third ** len(even)
        if len(odd) == 3:
            out.append(None)
        elif len(odd) == 2:
            out.append(rho * (vel[odd[0]] * vel[odd[1]] * scale))
        elif len(odd) == 1:
            out.append(rho * (vel[odd[0]] * scale))
        elif not even:
            out.append(rho)
        else:
            total = sq[even[0]]
            for k in even[1:]:
                total = total + sq[k]
            out.append(rho * (scale + 3.0 * scale * total))
    return out


def shifted(value, b, c):
    if c:
        value = pltpu.roll(value, c % 128, 1)
    if b:
        value = pltpu.roll(value, b % 8, 0)
    return value


def lane_gather(table, index):
    return jnp.take_along_axis(table, index, axis=1, mode="promise_in_bounds")


def row_of(ref, lead, row):
    return jnp.broadcast_to(ref[lead + (slice(row, row + 1), slice(None))], (8, 128))


def line(ref, row):
    return jnp.broadcast_to(ref[row], (8, 128))


def total_of(u, e):
    total = None
    for n in range(3):
        if e[n]:
            term = u[n] if e[n] > 0 else -u[n]
            total = term if total is None else total + term
    return total


def body(
    n_gx,
    n_gy,
    pop_h,
    relax_h,
    solid_h,
    cell_h,
    normal_h,
    count_s,
    ref_h,
    corner_h,
    cweight_h,
    out,
    relax_s,
    pop,
    solid,
    cell,
    normal,
    sref,
    corner,
    cweight,
    part,
    fields,
    blocked,
    sample,
    sample_in,
    solid_x,
    solid_y,
    solid_d,
    part_in,
    fields_in,
    rows,
    rows_in,
    rows_d,
    rolled,
    posts,
    edges,
    in_sem,
    tally,
    s_send,
    s_recv,
    h_send,
    h_recv,
    ready,
    whole,
):
    p = lax.axis_index("gx")
    q = lax.axis_index("gy")
    px = [lax.rem(p + n_gx + a, n_gx) for a in (-1, 0, 1)]
    qy = [lax.rem(q + n_gy + b, n_gy) for b in (-1, 0, 1)]
    around = [lax.rem(q + k, n_gy) for k in range(n_gy)]

    loads = [
        pltpu.make_async_copy(src, dst, in_sem.at[k])
        for k, (src, dst) in enumerate(
            [
                (pop_h, pop),
                (corner_h, corner),
                (cweight_h, cweight),
                (relax_h, relax_s),
                (cell_h, cell),
                (normal_h, normal),
                (ref_h, sref),
                (solid_h, solid),
            ]
        )
    ]
    for copy in loads:
        copy.start()

    barrier = pltpu.get_barrier_semaphore()
    by_distance = sorted(range(n_gy), key=lambda k: -min(k, n_gy - k))
    targets = [(a, k) for a in (1, 0, -1) for k in by_distance if a or k]
    for k in by_distance:
        pl.semaphore_signal(
            barrier, inc=1, device_id=(px[0], around[k]), device_id_type=MESH
        )
    row_id = lax.broadcasted_iota(I32, (8, 128), 0)

    pl.semaphore_wait(barrier, n_gy)
    for k in by_distance:
        pl.semaphore_signal(
            ready, inc=1, device_id=(px[2], around[k]), device_id_type=MESH
        )

    vel = []
    for copy in loads[:3]:
        copy.wait()
    for x in range(2):
        f = [pop[i, x] * weight[i] for i in range(27)]
        for axis in (2, 1, 0):
            f = along(f, axis, to_moments)
        rho = f[0]
        inv = 1.0 / rho
        u = [f[9] * inv, f[3] * inv, f[1] * inv]
        vel.append(u)
        fields[0, x] = rho
        for k in range(3):
            fields[k + 1, x] = u[k]

    for j in range(4):
        total = [jnp.zeros((8, 128), F32) for _ in range(3)]
        lanes = slice(128 * j, 128 * (j + 1))
        for k in range(8):
            where = jnp.broadcast_to(corner[0, 0, k : k + 1, lanes], (8, 128))
            share = jnp.broadcast_to(cweight[0, 0, k : k + 1, lanes], (8, 128))
            lane = where & 127
            mine = jnp.where((where >> 7) & 7 == row_id, share, 0.0)
            upper = where >= 1024
            for n in range(3):
                got = jnp.where(upper, lane_gather(vel[1][n], lane), lane_gather(vel[0][n], lane))
                total[n] = total[n] + mine * got
        for n in range(3):
            summed = jnp.sum(total[n], axis=0, keepdims=True)
            sample[3 * j + n] = summed
            if j == 0:
                sample[12 + n] = summed

    par = lax.rem(q, 2)

    def window(d):
        return 3 * lax.div(lax.rem(d + n_gy - 1, n_gy), 2)

    mine = window(q)
    for r in range(6):
        sample_in[(n_gy + q) * 6 + r] = sample[mine + r]

    def send(src, dst, send_sem, recv_sem, peer):
        pltpu.make_async_remote_copy(
            src_ref=src, dst_ref=dst, send_sem=send_sem, recv_sem=recv_sem,
            device_id=peer, device_id_type=MESH,
        ).start()

    def send_samples(a):
        for b, k in targets:
            if b == a:
                send(
                    sample.at[pl.ds(window(around[k]), 6)],
                    sample_in.at[pl.ds(((1 - a) * n_gy + q) * 6, 6)],
                    s_send,
                    s_recv.at[1 - a],
                    (px[a + 1], around[k]),
                )

    def send_side(n):
        a = 1 - 2 * n
        x = 1 - n
        to = px[a + 1]
        halo = []
        for m, b in enumerate((1, -1)):
            halo.append(
                (rows.at[pl.ds(42 * m + 24 + 9 * n, 9)], rows_d.at[pl.ds((2 * n + m) * 9, 9)], (to, qy[b + 1]))
            )
        halo.append((fields.at[:, x], fields_in.at[n], (to, q)))
        halo.append((part.at[pl.ds(18 - 18 * n, 9), x], part_in.at[n], (to, q)))
        halo.append((solid.at[x], solid_x.at[n], (to, q)))
        for m, b in enumerate((1, -1)):
            halo.append((solid.at[x], solid_d.at[n, m], (to, qy[b + 1])))
        for src, dst, peer in halo:
            send(src, dst, h_send, h_recv.at[n], peer)

    def send_row():
        for m, b in enumerate((1, -1)):
            to = (p, qy[b + 1])
            send(rows.at[pl.ds(42 * m, 24)], rows_in.at[pl.ds(24 * m, 24)], h_send, h_recv.at[2], to)
            send(solid, solid_y.at[m], h_send, h_recv.at[2], to)

    def arrived(sem, lines):
        span = tally.at[pl.ds(0, lines)]
        pltpu.make_async_copy(span, span, sem).wait()

    side_lines = 2 * 9 + 48 + 72 + 24
    row_lines = 2 * (24 + 16)

    odd = lax.rem(p, 2)
    pl.when(odd == 1)(lambda: send_samples(1))

    for copy in loads[4:]:
        copy.wait()
    cells = cell[0]
    live = lax.broadcasted_iota(I32, (1, 512), 1) < count_s[0, 0]
    refs = sref[0]
    first = jnp.where(live, (refs & 63) + 1, 0)
    second = jnp.where(live, (refs >> 6) * 8 + normal[0], 0)
    rows16 = lax.broadcasted_iota(I32, (16, 512), 0) == (cells >> 7)
    left = jnp.concatenate(
        [jnp.where(rows16, first, 0), jnp.where(rows16, second, 0)], axis=0
    ).astype(F32).astype(jnp.bfloat16)
    right = jnp.where(
        lax.broadcasted_iota(I32, (128, 512), 0) == (cells & 127), 1.0, 0.0
    ).astype(jnp.bfloat16)
    code = lax.dot_general(
        left, right, (((1,), (1,)), ((), ())), preferred_element_type=F32
    ).astype(I32)
    slot = code[0:16]
    owner = code[16:32]
    use = jnp.where(slot > 0, (owner >> 3) * 64 + slot, 0).astype(F32)
    axes = ((owner & 7) >> 1).astype(F32)
    for x in range(2):
        fields[4, x] = use[8 * x : 8 * x + 8]
        fields[5, x] = axes[8 * x : 8 * x + 8]

    loads[3].wait()
    for x in range(2):
        f = [pop[i, x] * weight[i] for i in range(27)]
        for axis in (2, 1, 0):
            f = along(f, axis, to_moments)
        balance = equilibrium_moments(fields[0, x], [fields[1 + k, x] for k in range(3)])
        for m in range(27):
            off = f[m] if balance[m] is None else f[m] - balance[m]
            f[m] = off * (1.0 - relax_s[m])
        for axis in (2, 1, 0):
            f = along(f, axis, from_moments)
        for i, e in enumerate(steps):
            part[i, x] = f[i] * float(np.prod([1.5 if v == 0 else 3.0 for v in e]))

    for m, b in enumerate((1, -1)):
        near = slice(7, 8) if b == 1 else slice(0, 1)
        base = 42 * m
        for c in (-1, 0, 1):
            for s, (a, x) in enumerate(((0, 0), (0, 1), (1, 0), (-1, 1))):
                rows[base + 4 * (c + 1) + s] = part[index_of[a, b, c], x, near]
            for n, (a, x) in enumerate(((1, 1), (-1, 0))):
                rows[base + 24 + 9 * n + c + 1] = part[index_of[a, b, c], x, near]
        for k in range(6):
            for x in range(2):
                value = fields[k, x, near]
                rows[base + 12 + 6 * x + k] = value
                rows[base + 27 + 9 * (1 - x) + k] = value

    send_side(0)
    pl.when(odd == 0)(lambda: send_samples(1))
    def greet():
        pl.semaphore_wait(ready, n_gy)
        pl.semaphore_signal(whole, inc=1, device_id=(px[0], q), device_id_type=MESH)

    def send_back():
        send_samples(-1)
        send_side(1)

    pl.when(p != 0)(greet)
    pl.semaphore_wait(whole, 1)
    send_samples(0)
    send_row()
    pl.when(p != 0)(send_back)

    chunk = [0, 1 - par, 1]
    half = [1 - par, par, 1 - par]

    def table(g, t, k, n):
        return line(sample_in, (g * n_gy + around[k]) * 6 + 3 * chunk[t] + n)

    def wall_velocity(use, axis, u, tables, lanes):
        use = use.astype(I32)
        spot = use - 1
        who = spot >> 6
        lane = (spot & 63) + lanes
        picked = [jnp.zeros((8, 128), F32) for _ in range(3)]
        for k in reversed(by_distance):
            here = who == around[k]
            for n in range(3):
                picked[n] = jnp.where(here, lane_gather(tables(k, n), lane), picked[n])
        return [
            jnp.where(use > 0, jnp.where(axis == float(n), 0.0, wall_ratio * picked[n]), u[n])
            for n in range(3)
        ]

    def base_of(rho, u):
        return rho - 1.5 * rho * (u[0] * u[0] + u[1] * u[1] + u[2] * u[2])

    arrived(s_recv.at[1], (n_gy - 1) * 6)
    for x in range(2):
        rho = fields[0, x]
        u = wall_velocity(
            fields[4, x], fields[5, x], [fields[1 + n, x] for n in range(3)],
            lambda k, n: table(1, 1, k, n), half[1] * 64,
        )
        base = base_of(rho, u)
        for i in range(13, 27):
            along_e = total_of(u, steps[i])
            if along_e is None:
                posts[i, x] = part[i, x] + base
                continue
            linear = 3.0 * rho * along_e
            even = base + 1.5 * along_e * linear
            posts[i, x] = part[i, x] + (even + linear)
            posts[26 - i, x] = part[26 - i, x] + (even - linear)
    for i, (a, b, c) in enumerate(steps):
        for x in range(2):
            if 0 <= x + a <= 1:
                rolled[i, x] = shifted(posts[i, x], b, c)

    def side(n):
        a = 1 - 2 * n
        rho = fields_in[n, 0]
        u = wall_velocity(
            fields_in[n, 4], fields_in[n, 5], [fields_in[n, 1 + k] for k in range(3)],
            lambda k, m: table(2 * n, 1, k, m), half[1] * 64,
        )
        base = base_of(rho, u)
        for s, (b, c) in enumerate((b, c) for b in (-1, 0, 1) for c in (-1, 0, 1)):
            along_e = total_of(u, (a, b, c))
            linear = 3.0 * rho * along_e
            value = part_in[n, s] + (base + linear + 1.5 * along_e * linear)
            rolled[index_of[a, b, c], 1 - n] = shifted(value, b, c)

    def block_plane(xx, plane):
        for b in (-1, 0, 1):
            moved = plane
            if b:
                m = 0 if b == 1 else 1
                near = 7 if b == 1 else 0
                if xx in (1, 2):
                    edge = row_of(solid_y, (m, xx - 1), near)
                else:
                    edge = row_of(solid_d, (0 if xx == 0 else 1, m), near)
                moved = pltpu.roll(plane, b % 8, 0)
                moved = jnp.where(row_id == (0 if b == 1 else 7), edge, moved)
            for c in (-1, 0, 1):
                blocked[xx, 3 * (b + 1) + c + 1] = shifted(moved, 0, c)

    at = [row_id == s for s in range(8)]
    lower = row_id < 4
    across = row_id & 3

    def gather_rows(entries):
        value = None
        for s, piece in entries:
            value = piece if value is None else jnp.where(at[s], piece, value)
        return value

    def field_row(k, near):
        entries = []
        for m in range(2):
            if near:
                entries.append((4 * m + 1, line(rows_in, m * 24 + 12 + k)))
                entries.append((4 * m + 2, line(rows_in, m * 24 + 18 + k)))
                entries.append((4 * m + 3, line(rows_d, (2 + m) * 9 + 3 + k)))
            else:
                entries.append((4 * m, line(rows_d, m * 9 + 3 + k)))
        return gather_rows(entries)

    def part_row(a, c, near):
        entries = []
        for m in range(2):
            base = m * 24 + 4 * (c + 1)
            if not near:
                entries.append((4 * m, line(rows_d, m * 9 + c + 1)))
            elif a == 0:
                entries.append((4 * m + 1, line(rows_in, base)))
                entries.append((4 * m + 2, line(rows_in, base + 1)))
            elif a == 1:
                entries.append((4 * m + 1, line(rows_in, base + 2)))
            else:
                entries.append((4 * m + 2, line(rows_in, base + 3)))
                entries.append((4 * m + 3, line(rows_d, (2 + m) * 9 + c + 1)))
        return gather_rows(entries)

    def table_near(k, n):
        value = jnp.where(lower, table(1, 0, k, n), table(1, 2, k, n))
        other = jnp.where(lower, table(2, 0, k, n), table(2, 2, k, n))
        return jnp.where(across == 3, other, value)

    def table_far(k, n):
        return jnp.where(lower, table(0, 0, k, n), table(0, 2, k, n))

    def edge_rows(found, parts, tables, where):
        rho = found[0]
        u = wall_velocity(found[4], found[5], found[1:4], tables, (1 - par) * 64)
        base = base_of(rho, u)
        u = [u[0], jnp.where(lower, u[1], -u[1]), u[2]]
        for (a, c), piece in parts.items():
            along_e = total_of(u, (a, 1, c))
            linear = 3.0 * rho * along_e
            value = piece + (base + linear + 1.5 * along_e * linear)
            edges[where + 3 * (a + 1) + c + 1] = shifted(value, 0, c)

    def finish(far):
        for i, (a, b, c) in enumerate(steps):
            for x in range(2):
                xx = x - a
                if (xx == -1) != far:
                    continue
                value = rolled[i, xx if 0 <= xx <= 1 else 1 if a == 1 else 0]
                if b:
                    m = 0 if b == 1 else 1
                    s = (9 if far else 0) + 3 * (a + 1) + c + 1
                    edge = row_of(edges, (s,), 4 * m + xx + 1)
                    value = jnp.where(row_id == (0 if b == 1 else 7), edge, value)
                wall = blocked[xx + 1, 3 * (b + 1) + c + 1]
                out[i, x] = jnp.where(wall != 0, posts[26 - i, x], value)

    arrived(h_recv.at[2], row_lines)
    arrived(h_recv.at[1], side_lines)
    for xx, plane in ((1, solid[0]), (2, solid[1]), (3, solid_x[1])):
        block_plane(xx, plane)
    found = [field_row(k, True) for k in range(6)]
    parts = {(a, c): part_row(a, c, True) for a in (-1, 0, 1) for c in (-1, 0, 1)}
    arrived(s_recv.at[2], n_gy * 6)
    side(1)
    edge_rows(found, parts, table_near, 0)
    finish(False)

    @pl.when(p == 0)
    def _():
        greet()
        send_back()

    arrived(h_recv.at[0], side_lines)
    block_plane(0, solid_x[0])
    found = [field_row(k, False) for k in range(6)]
    parts = {(1, c): part_row(1, c, False) for c in (-1, 0, 1)}
    arrived(s_recv.at[0], n_gy * 6)
    side(0)
    edge_rows(found, parts, table_far, 9)
    finish(True)

    arrived(s_send, len(targets) * 6)
    arrived(h_send, 2 * side_lines + row_lines)


def local(*args):
    n_gx, n_gy = lax.axis_size("gx"), lax.axis_size("gy")
    hbm = pl.BlockSpec(memory_space=pl.ANY)
    smem = pl.BlockSpec(memory_space=pltpu.SMEM)
    vmem = pltpu.VMEM
    dma = pltpu.SemaphoreType.DMA
    args = [
        a if k == 5 else pltpu.with_memory_space_constraint(a, pltpu.HBM)
        for k, a in enumerate(args)
    ]
    return pl.pallas_call(
        lambda *refs: body(n_gx, n_gy, *refs),
        name="lattice_step",
        out_shape=vmem((27, 2, 8, 128), F32),
        in_specs=[hbm, hbm, hbm, hbm, hbm, smem, hbm, hbm, hbm],
        out_specs=pl.BlockSpec(memory_space=pltpu.VMEM),
        scratch_shapes=[
            pltpu.SMEM((27,), F32),
            vmem((27, 2, 8, 128), F32),
            vmem((2, 8, 128), I32),
            vmem((1, 1, 512), I32),
            vmem((1, 1, 512), I32),
            vmem((1, 1, 512), I32),
            vmem((1, 1, 8, 512), I32),
            vmem((1, 1, 8, 512), F32),
            vmem((27, 2, 8, 128), F32),
            vmem((6, 2, 8, 128), F32),
            vmem((4, 9, 8, 128), I32),
            vmem((15, 1, 128), F32),
            vmem((3 * n_gy * 6, 1, 128), F32),
            vmem((2, 8, 128), I32),
            vmem((2, 2, 8, 128), I32),
            vmem((2, 2, 8, 128), I32),
            vmem((2, 9, 8, 128), F32),
            vmem((2, 6, 8, 128), F32),
            vmem((84, 1, 128), F32),
            vmem((48, 1, 128), F32),
            vmem((36, 1, 128), F32),
            vmem((27, 2, 8, 128), F32),
            vmem((27, 2, 8, 128), F32),
            vmem((18, 8, 128), F32),
            dma((8,)),
            vmem((404, 1, 128), F32),
            dma(()),
            dma((3,)),
            dma(()),
            dma((3,)),
            pltpu.SemaphoreType.REGULAR,
            pltpu.SemaphoreType.REGULAR,
        ],
        compiler_params=pltpu.CompilerParams(
            collective_id=0, has_side_effects=True, vmem_limit_bytes=16 << 20
        ),
    )(*args)


def solution(mesh):
    return jax.shard_map(
        local,
        mesh=mesh,
        in_specs=(
            P(None, "gx", "gy", None),
            P(),
            P("gx", "gy", None),
            P("gx", "gy", None),
            P("gx", "gy", None),
            P("gx", "gy"),
            P("gx", "gy", None),
            P("gx", "gy", None, None),
            P("gx", "gy", None, None),
        ),
        out_specs=P(None, "gx", "gy", None),
        check_vma=False,
    )
```
